16 devices in a mesh: tp: 2 (over z), dp: 8 (over y, x, core).
Axes of the slice: x: 2, y: 2, z: 2, core: 2. Of those that a mesh axis runs over, the one named last changes fastest.
Arguments:
- h_main: bfloat16 [8, 512, 2048], P('dp')
- h_mtp: bfloat16 [8, 512, 2048], P('dp')
- labels_main: int32 [8, 512], P('dp')
- labels_mtp: int32 [8, 512], P('dp')
- weight_main: float32 [8, 512], P('dp')
- weight_mtp: float32 [8, 512], P('dp')
- gain_final: float32 [2048], replicated
- gain_mtp: float32 [2048], replicated
- w_out: bfloat16 [2048, 32256], P(None, 'tp')
Outputs:
- output 1: float32 [], replicated
- output 2: bfloat16 [8, 512, 2048], P('dp')
- output 3: bfloat16 [8, 512, 2048], P('dp')
- output 4: float32 [2048, 32256], P('dp', 'tp')
- output 5: float32 [2048], replicated
- output 6: float32 [2048], replicated
All inputs are finite; a program needn't handle non-finite values.
Results may differ from the reference program's by a relative error of at most 0.00844002.
Values sent between devices are 32-bit elements.
A program may use at most 1 GiB of HBM per device.

```python
import jax
import jax.numpy as jnp
from jax import lax

BATCH_ALL = 8
SEQ_LEN = 512
D_MODEL = 2048
VOCAB_SIZE = 32256
TP_SHARDS = 2
ROW_BLOCK = 256
SHARD_VOCAB = VOCAB_SIZE // TP_SHARDS
ROWS_ALL = BATCH_ALL * SEQ_LEN
NUM_BLOCKS = ROWS_ALL // ROW_BLOCK
NORM_EPS = 1e-6
MTP_LAMBDA = 0.3
LOGIT_SCALE = 3.0


def setup_inputs(seed: int = 0) -> dict:
    key_list = jax.random.split(jax.random.key(seed), 7)
    h_main = jax.random.normal(key_list[0], (BATCH_ALL, SEQ_LEN, D_MODEL), jnp.float32).astype(jnp.bfloat16)
    h_mtp = jax.random.normal(key_list[1], (BATCH_ALL, SEQ_LEN, D_MODEL), jnp.float32).astype(jnp.bfloat16)
    tokens = jax.random.randint(key_list[2], (BATCH_ALL, SEQ_LEN + 2), 0, VOCAB_SIZE, jnp.int32)
    tokens = tokens.at[0, 1].set(VOCAB_SIZE - 1).at[0, 2].set(0)
    lengths = jax.random.randint(key_list[3], (BATCH_ALL,), SEQ_LEN // 4, SEQ_LEN + 1, jnp.int32)
    lengths = lengths.at[0].set(SEQ_LEN).at[BATCH_ALL - 1].set(SEQ_LEN // 4)
    positions = jnp.arange(SEQ_LEN, dtype=jnp.int32)[None, :]
    weight_main = (positions < lengths[:, None]).astype(jnp.float32)
    weight_mtp = (positions < lengths[:, None] - 1).astype(jnp.float32)
    gain_final = 1.0 + 0.2 * jax.random.normal(key_list[4], (D_MODEL,), jnp.float32)
    gain_mtp = 1.0 + 0.2 * jax.random.normal(key_list[5], (D_MODEL,), jnp.float32)
    w_out = (jax.random.normal(key_list[6], (D_MODEL, VOCAB_SIZE), jnp.float32) * (LOGIT_SCALE * D_MODEL ** -0.5)).astype(jnp.bfloat16)
    return {"h_main": h_main, "h_mtp": h_mtp, "labels_main": tokens[:, 1:SEQ_LEN + 1], "labels_mtp": tokens[:, 2:], "weight_main": weight_main, "weight_mtp": weight_mtp, "gain_final": gain_final, "gain_mtp": gain_mtp, "w_out": w_out}


def norm_apply(x_rows, gain_vec):
    return x_rows * lax.rsqrt(jnp.mean(x_rows * x_rows, axis=-1, keepdims=True) + NORM_EPS) * gain_vec


def reference(h_main, h_mtp, labels_main, labels_mtp, weight_main, weight_mtp, gain_final, gain_mtp, w_out):
    coef_main = 1.0 / jnp.sum(weight_main)
    coef_mtp = MTP_LAMBDA / jnp.sum(weight_mtp)
    x_blocks = jnp.stack([h_main, h_mtp]).astype(jnp.float32).reshape(2 * NUM_BLOCKS, ROW_BLOCK, D_MODEL)
    label_blocks = jnp.stack([labels_main, labels_mtp]).reshape(2 * NUM_BLOCKS, ROW_BLOCK)
    weight_blocks = jnp.stack([weight_main * coef_main, weight_mtp * coef_mtp]).reshape(2 * NUM_BLOCKS, ROW_BLOCK)
    gain_blocks = jnp.repeat(jnp.stack([gain_final, gain_mtp]), NUM_BLOCKS, axis=0)
    w_shards = w_out.reshape(D_MODEL, TP_SHARDS, SHARD_VOCAB).transpose(1, 0, 2)

    def shard_product(operand_pair):
        grad_shard, w_shard = operand_pair
        return jnp.dot(grad_shard, w_shard.T, preferred_element_type=jnp.float32).astype(jnp.bfloat16)

    def block_step(grad_w, block_data):
        x_rows, labels, row_w, gain_vec = block_data
        u_rows = norm_apply(x_rows, gain_vec).astype(jnp.bfloat16)
        logits = jnp.dot(u_rows, w_out, preferred_element_type=jnp.float32)
        row_max = jnp.max(logits, axis=-1, keepdims=True)
        log_norm = row_max + jnp.log(jnp.sum(jnp.exp(logits - row_max), axis=-1, keepdims=True))
        onehot = jax.nn.one_hot(labels, VOCAB_SIZE, dtype=jnp.float32)
        target = jnp.sum(logits * onehot, axis=-1)
        loss_part = jnp.sum(row_w * (log_norm[:, 0] - target))
        grad_z = (row_w[:, None] * (jnp.exp(logits - log_norm) - onehot)).astype(jnp.bfloat16)
        grad_w = grad_w + lax.dot_general(u_rows, grad_z, (((0,), (0,)), ((), ())), preferred_element_type=jnp.float32)
        grad_split = grad_z.reshape(ROW_BLOCK, TP_SHARDS, SHARD_VOCAB).transpose(1, 0, 2)
        partials = lax.map(shard_product, (grad_split, w_shards))
        grad_u = jnp.sum(partials.astype(jnp.float32), axis=0)
        _, norm_vjp = jax.vjp(norm_apply, x_rows, gain_vec)
        grad_x, grad_gain = norm_vjp(grad_u)
        return grad_w, (loss_part, grad_x.astype(jnp.bfloat16), grad_gain)

    grad_w, outputs = lax.scan(block_step, jnp.zeros((D_MODEL, VOCAB_SIZE), jnp.float32), (x_blocks, label_blocks, weight_blocks, gain_blocks))
    loss_parts, grad_x, grad_gain = outputs
    grad_h = grad_x.reshape(2, BATCH_ALL, SEQ_LEN, D_MODEL)
    gain_grads = grad_gain.reshape(2, NUM_BLOCKS, D_MODEL).sum(axis=1)
    return (jnp.sum(loss_parts), grad_h[0], grad_h[1], grad_w, gain_grads[0], gain_grads[1])
```

```python
import functools

import jax
import jax.numpy as jnp
from jax import lax
from jax.experimental import pallas as pl
from jax.experimental.pallas import tpu as pltpu
from jax.sharding import PartitionSpec as P


NORM_EPS = 1e-6
MTP_LAMBDA = 0.3
BLOCK_COLS = 4096
TILE = 2304
NARROW = 256
VMEM_LIMIT = 60 * 1024 * 1024
NN = (((1,), (0,)), ((), ()))
NT = (((1,), (1,)), ((), ()))


def params(*semantics):
    return pltpu.CompilerParams(dimension_semantics=semantics, vmem_limit_bytes=VMEM_LIMIT)


HBM = pl.BlockSpec(memory_space=pl.ANY)


def norm_kernel(tp_ref, h0_ref, h1_ref, gain_ref, _, u_ref, near_ref, c0_ref, c1a_ref, c1b_ref):
    head, b = pl.program_id(0), pl.program_id(1)

    def rows_of(h_ref):
        x = h_ref[0].astype(jnp.float32)
        return x * lax.rsqrt(jnp.mean(x * x, axis=-1, keepdims=True) + NORM_EPS)

    for i, h_ref in enumerate((h0_ref, h1_ref)):
        @pl.when(head == i)
        def _():
            u = rows_of(h_ref) * gain_ref[i:i + 1, :]
            u_ref[...] = u.astype(jnp.bfloat16)

            @pl.when(b == tp_ref[0])
            def _():
                near_ref[...] = u

            if i == 0:
                @pl.when(b >= 2)
                def _():
                    c0_ref[...] = u
            else:
                @pl.when(b == 2)
                def _():
                    c1a_ref[...] = u

                @pl.when(b == 3)
                def _():
                    c1b_ref[...] = u


def run_norm(tp, h0, h1, gains, dep):
    _, rows, d = h0.shape
    q = rows // 4
    f32 = jnp.float32
    blk = lambda f: pl.BlockSpec((q, d), f)
    return pl.pallas_call(
        norm_kernel,
        out_shape=(jax.ShapeDtypeStruct((2 * rows, d), jnp.bfloat16), jax.ShapeDtypeStruct((2 * q, d), f32), jax.ShapeDtypeStruct((2 * q, d), f32), jax.ShapeDtypeStruct((q, d), f32), jax.ShapeDtypeStruct((q, d), f32)),
        grid_spec=pltpu.PrefetchScalarGridSpec(
            num_scalar_prefetch=1, grid=(2, 4),
            in_specs=[pl.BlockSpec((1, q, d), lambda h, b, s: (0, jnp.where(h == 0, b, 3), 0)), pl.BlockSpec((1, q, d), lambda h, b, s: (0, jnp.where(h == 0, 0, b), 0)), pl.BlockSpec((2, d), lambda h, b, s: (0, 0)), HBM],
            out_specs=(blk(lambda h, b, s: (4 * h + b, 0)), blk(lambda h, b, s: (h, 0)), blk(lambda h, b, s: (jnp.where(h == 0, jnp.maximum(b - 2, 0), 1), 0)), blk(lambda h, b, s: (0, 0)), blk(lambda h, b, s: (0, 0)))),
        compiler_params=params("arbitrary", "arbitrary"),
        cost_estimate=pl.CostEstimate(flops=8 * rows * d * 1000, bytes_accessed=14 * rows * d, transcendentals=rows),
        name="norm",
    )(tp, h0, h1, gains, dep)


def norm_back_kernel(h_ref, a_ref, b_ref, gain_ref, _, out_ref, gg_ref):
    @pl.when(pl.program_id(0) == 0)
    def _():
        gg_ref[...] = jnp.zeros_like(gg_ref)

    x = h_ref[0].astype(jnp.float32)
    inv = lax.rsqrt(jnp.mean(x * x, axis=-1, keepdims=True) + NORM_EPS)
    normed = x * inv
    gu = a_ref[...] + b_ref[...]
    gn = gu * gain_ref[...]
    prod = gu * normed
    gg_ref[...] += jnp.sum(prod, axis=0, keepdims=True)
    gx = inv * (gn - normed * jnp.mean(gn * normed, axis=-1, keepdims=True))
    out_ref[0] = gx.astype(jnp.bfloat16)


def run_norm_back(h, a, b, gain, dep):
    _, rows, d = h.shape
    q = 128
    row = pl.BlockSpec((q, d), lambda i: (i, 0))
    row3 = pl.BlockSpec((1, q, d), lambda i: (0, i, 0))
    one = pl.BlockSpec((1, d), lambda i: (0, 0))
    return pl.pallas_call(
        norm_back_kernel,
        out_shape=(jax.ShapeDtypeStruct(h.shape, jnp.bfloat16), jax.ShapeDtypeStruct((1, d), jnp.float32)),
        grid=(rows // q,),
        in_specs=[row3, row, row, one, HBM],
        out_specs=(row3, one),
        compiler_params=params("arbitrary"),
        cost_estimate=pl.CostEstimate(flops=8 * rows * d * 1000, bytes_accessed=12 * rows * d, transcendentals=rows),
        name="norm_back",
    )(h, a, b, gain, dep)


def logits_kernel(start_ref, u_ref, w_ref, lab_ref, _, z_ref, stat_ref, m_ref, s_ref, t_ref, *, sub):
    j = pl.program_id(0)
    rows, tile = z_ref.shape
    lanes = 128

    @pl.when(j == 0)
    def _():
        m_ref[...] = jnp.full_like(m_ref, -jnp.inf)
        s_ref[...] = jnp.zeros_like(s_ref)
        t_ref[...] = jnp.zeros_like(t_ref)

    base = start_ref[0] + j * tile
    z_ref[...] = lax.dot_general(u_ref[...], w_ref[...], NN, preferred_element_type=jnp.float32)
    for i in range(rows // sub):
        r = pl.ds(i * sub, sub)
        z = z_ref[r, :]
        lab = lab_ref[r, :] - base
        parts = [z[:, k * lanes:(k + 1) * lanes] for k in range(tile // lanes)]
        m_old = m_ref[r, :]
        m_new = m_old
        for p in parts:
            m_new = jnp.maximum(m_new, p)
        lane = lax.broadcasted_iota(jnp.int32, (sub, lanes), 1)
        off = lab - lane
        total = s_ref[r, :] * jnp.exp(m_old - m_new)
        target = t_ref[r, :]
        for k, p in enumerate(parts):
            total += jnp.exp(p - m_new)
            target = jnp.where(off == k * lanes, p, target)
        m_ref[r, :] = m_new
        s_ref[r, :] = total
        t_ref[r, :] = target

    @pl.when(j == pl.num_programs(0) - 1)
    def _():
        m = m_ref[...]
        top = jnp.max(m, axis=1, keepdims=True)
        stat_ref[0] = top
        stat_ref[1] = jnp.sum(s_ref[...] * jnp.exp(m - top), axis=1, keepdims=True)
        stat_ref[2] = jnp.sum(t_ref[...], axis=1, keepdims=True)


def run_logits(start, u, w, lab, dep, head, rows):
    d, cols = w.shape
    return pl.pallas_call(
        functools.partial(logits_kernel, sub=128),
        out_shape=(jax.ShapeDtypeStruct((rows, cols), jnp.float32), jax.ShapeDtypeStruct((3, rows, 1), jnp.float32)),
        grid_spec=pltpu.PrefetchScalarGridSpec(
            num_scalar_prefetch=1, grid=(cols // TILE,),
            in_specs=[pl.BlockSpec((rows, d), lambda j, s: (head, 0)), pl.BlockSpec((d, TILE), lambda j, s: (0, j)), pl.BlockSpec((rows, 1), lambda j, s: (head, 0)), HBM],
            out_specs=(pl.BlockSpec((rows, TILE), lambda j, s: (0, j)), pl.BlockSpec((3, rows, 1), lambda j, s: (0, 0, 0))),
            scratch_shapes=[pltpu.VMEM((rows, 128), jnp.float32)] * 3),
        compiler_params=params("arbitrary"),
        cost_estimate=pl.CostEstimate(flops=2 * rows * d * cols, bytes_accessed=cols * (2 * d + 4 * rows), transcendentals=rows * cols),
        name="logits",
    )(start, u, w, lab, dep)


def e_tile(z, shift, weight, off):
    parts = []
    for k in range(z.shape[1] // 128):
        p = jnp.exp(z[:, k * 128:(k + 1) * 128] - shift)
        parts.append(jnp.where(off == k * 128, p - weight, p))
    return jnp.concatenate(parts, axis=1).astype(jnp.bfloat16)


def fill_rows(vals_ref, norm_ref, wt_ref, lab_ref, shift_ref, weight_ref, off_ref):
    shape = shift_ref.shape
    wt = wt_ref[...]
    shift_ref[...] = jnp.broadcast_to(norm_ref[...] - jnp.log(wt), shape)
    weight_ref[...] = jnp.broadcast_to(wt, shape)
    off_ref[...] = lab_ref[...] - vals_ref[0] - lax.broadcasted_iota(jnp.int32, shape, 1)


def row_scratch(rows):
    return [pltpu.VMEM((rows, 128), jnp.float32), pltpu.VMEM((rows, 128), jnp.float32), pltpu.VMEM((rows, 128), jnp.int32)]


def du_kernel(start_ref, z_ref, w_ref, norm_ref, wt_ref, lab_ref, _, out_ref, acc_ref, shift_ref, weight_ref, off_ref):
    j = pl.program_id(0)

    @pl.when(j == 0)
    def _():
        acc_ref[...] = jnp.zeros_like(acc_ref)
        fill_rows(start_ref, norm_ref, wt_ref, lab_ref, shift_ref, weight_ref, off_ref)

    e = e_tile(z_ref[...], shift_ref[...], weight_ref[...], off_ref[...] - j * z_ref.shape[1])
    acc_ref[...] += lax.dot_general(e, w_ref[...], NT, preferred_element_type=jnp.float32)

    @pl.when(j == pl.num_programs(0) - 1)
    def _():
        out_ref[...] = acc_ref[...].astype(jnp.bfloat16).astype(jnp.float32)


def run_du(start, z, w, norm, wt, lab, dep, head, rows):
    d, cols = w.shape
    steps = cols // TILE
    vec = pl.BlockSpec((rows, 1), lambda j, s: (head, 0))
    return pl.pallas_call(
        du_kernel,
        out_shape=jax.ShapeDtypeStruct((rows, d), jnp.float32),
        grid_spec=pltpu.PrefetchScalarGridSpec(
            num_scalar_prefetch=1, grid=(steps,),
            in_specs=[pl.BlockSpec((rows, TILE), lambda j, s: (0, j)), pl.BlockSpec((d, TILE), lambda j, s: (0, j)), vec, vec, vec, HBM],
            out_specs=pl.BlockSpec((rows, d), lambda j, s: (0, 0)),
            scratch_shapes=[pltpu.VMEM((rows, d), jnp.float32)] + row_scratch(rows)),
        compiler_params=params("arbitrary"),
        cost_estimate=pl.CostEstimate(flops=2 * rows * d * cols, bytes_accessed=cols * (2 * d + 4 * rows), transcendentals=rows * cols),
        name="du",
    )(start, z, w, norm, wt, lab, dep)


def own_e_kernel(start_ref, z0_ref, z1_ref, u_ref, norm_ref, wt_ref, lab_ref, e_ref, uo_ref, shift_ref, weight_ref, off_ref):
    j = pl.program_id(0)

    @pl.when(j == 0)
    def _():
        fill_rows(start_ref, norm_ref, wt_ref, lab_ref, shift_ref, weight_ref, off_ref)

    uo_ref[...] = u_ref[...]
    rows = z0_ref.shape[0]
    at = (start_ref[1] + j) * NARROW
    for i, z_ref in enumerate((z0_ref, z1_ref)):
        r = slice(i * rows, (i + 1) * rows)
        e_ref[r, :] = e_tile(z_ref[...], shift_ref[r, :], weight_ref[r, :], off_ref[r, :] - at)


def run_own_e(start, z0, z1, u, norm, wt, lab):
    rows, d = u.shape
    steps = BLOCK_COLS // NARROW
    vec = pl.BlockSpec((rows, 1), lambda j, s: (0, 0))
    u_spec = pl.BlockSpec((rows // steps, d), lambda j, s: (j, 0))
    z_spec = pl.BlockSpec((rows // 2, NARROW), lambda j, s: (0, s[1] + j))
    return pl.pallas_call(
        own_e_kernel,
        out_shape=(jax.ShapeDtypeStruct((4 * rows, BLOCK_COLS), jnp.bfloat16), jax.ShapeDtypeStruct((4 * rows, d), jnp.bfloat16)),
        grid_spec=pltpu.PrefetchScalarGridSpec(
            num_scalar_prefetch=1, grid=(steps,),
            in_specs=[z_spec, z_spec, u_spec, vec, vec, vec],
            out_specs=(pl.BlockSpec((rows, NARROW), lambda j, s: (0, j)), u_spec),
            scratch_shapes=row_scratch(rows)),
        compiler_params=params("arbitrary"),
        cost_estimate=pl.CostEstimate(flops=rows * BLOCK_COLS * 2048, bytes_accessed=rows * (6 * BLOCK_COLS + 4 * d), transcendentals=rows * BLOCK_COLS),
        name="own_e",
    )(start, z0, z1, u, norm, wt, lab)


def class_e_kernel(start_ref, *refs):
    n = len(refs) - 12
    pieces, (w0_ref, w1_ref, norm_ref, wt_ref, lab_ref, _, _, e_ref, u_ref, shift_ref, weight_ref, off_ref) = refs[:n], refs[n:]
    j = pl.program_id(0)

    @pl.when(j == 0)
    def _():
        at = 0
        for p in pieces:
            u_ref[at:at + p.shape[0], :] = p[...].astype(jnp.bfloat16)
            at += p.shape[0]
        fill_rows(start_ref, norm_ref, wt_ref, lab_ref, shift_ref, weight_ref, off_ref)

    for i, w_ref in enumerate((w0_ref, w1_ref)):
        z = lax.dot_general(u_ref[...], w_ref[...], NN, preferred_element_type=jnp.float32)
        at = (start_ref[1] + 2 * j + i) * NARROW
        e_ref[:, i * NARROW:(i + 1) * NARROW] = e_tile(z, shift_ref[...], weight_ref[...], off_ref[...] - at)


def run_class_e(start, pieces, w, norm, wt, lab, e_all, u_all, slot):
    d = w.shape[0]
    rows = sum(p.shape[0] for p in pieces)
    full = lambda j, s: (0, 0)
    once = pl.Buffered(1)
    vec = pl.BlockSpec((rows, 1), full)
    n = len(pieces)
    return pl.pallas_call(
        class_e_kernel,
        out_shape=(jax.ShapeDtypeStruct(e_all.shape, e_all.dtype), jax.ShapeDtypeStruct(u_all.shape, u_all.dtype)),
        grid_spec=pltpu.PrefetchScalarGridSpec(
            num_scalar_prefetch=1, grid=(BLOCK_COLS // (2 * NARROW),),
            in_specs=[pl.BlockSpec(p.shape, full, pipeline_mode=once) for p in pieces] + [pl.BlockSpec((d, NARROW), lambda j, s: (0, s[1] + 2 * j)), pl.BlockSpec((d, NARROW), lambda j, s: (0, s[1] + 2 * j + 1)), vec, vec, vec, HBM, HBM],
            out_specs=(pl.BlockSpec((rows, 2 * NARROW), lambda j, s: (slot, j)), pl.BlockSpec((rows, d), lambda j, s: (slot, 0))),
            scratch_shapes=row_scratch(rows)),
        input_output_aliases={1 + n + 5: 0, 1 + n + 6: 1},
        compiler_params=params("arbitrary"),
        cost_estimate=pl.CostEstimate(flops=2 * rows * d * BLOCK_COLS, bytes_accessed=BLOCK_COLS * 2 * (d + rows) + 6 * rows * d, transcendentals=rows * BLOCK_COLS),
        name="class_e",
    )(start, *pieces, w, w, norm, wt, lab, e_all, u_all)


def grad_w_kernel(start_ref, u_ref, e_ref, _, keep_ref, give_ref, ut_ref):
    @pl.when(pl.program_id(0) == 0)
    def _():
        ut_ref[...] = u_ref[...].T

    g = lax.dot_general(ut_ref[...], e_ref[...], NN, preferred_element_type=jnp.float32)
    half = g.shape[0] // 2

    @pl.when(start_ref[0] == 0)
    def _():
        keep_ref[...] = g[:half]
        give_ref[...] = g[half:]

    @pl.when(start_ref[0] == 1)
    def _():
        keep_ref[...] = g[half:]
        give_ref[...] = g[:half]


def run_grad_w(where, u_all, e_all, dep):
    rows, cols = e_all.shape
    blk, tn = 512, 512
    out = pl.BlockSpec((blk // 2, tn), lambda j, s: (0, j))
    return pl.pallas_call(
        grad_w_kernel,
        out_shape=(jax.ShapeDtypeStruct((blk // 2, cols), jnp.float32),) * 2,
        grid_spec=pltpu.PrefetchScalarGridSpec(
            num_scalar_prefetch=1, grid=(cols // tn,),
            in_specs=[pl.BlockSpec((rows, blk), lambda j, s: (0, s[1])), pl.BlockSpec((rows, tn), lambda j, s: (0, j)), HBM],
            out_specs=(out, out),
            scratch_shapes=[pltpu.VMEM((blk, rows), jnp.bfloat16)]),
        compiler_params=params("arbitrary"),
        cost_estimate=pl.CostEstimate(flops=2 * rows * blk * cols, bytes_accessed=2 * rows * (blk + cols) + 4 * blk * cols, transcendentals=0),
        name="grad_w",
    )(where, u_all, e_all, dep)


def place_kernel(at_ref, *refs, n, chunks):
    blocks, out_ref, bufs, in_sem, out_sem = refs[:n], refs[-n - 3], refs[-n - 2:-2], refs[-2], refs[-1]
    _, cols = blocks[0].shape
    width = cols // chunks
    at = at_ref[0] * NARROW

    def load(i, k):
        c = pl.ds(k * width, width)
        return pltpu.make_async_copy(blocks[i].at[:, c], bufs[i].at[:, c], in_sem.at[i, k])

    def store(k):
        to = pl.ds(pl.multiple_of(at + k * width, NARROW), width)
        return pltpu.make_async_copy(bufs[0].at[:, pl.ds(k * width, width)], out_ref.at[:, to], out_sem.at[k])

    for k in range(chunks):
        for i in range(n):
            load(i, k).start()
    for k in range(chunks):
        for i in range(n):
            load(i, k).wait()
        if n == 2:
            c = pl.ds(k * width, width)
            bufs[0][:, c] += bufs[1][:, c]
        store(k).start()
    for k in range(chunks):
        store(k).wait()


def run_place(at, blocks, out, dep, shape):
    rows, cols = blocks[0].shape
    n, chunks = len(blocks), 4
    extra = [dep] if out is None else [out, dep]
    return pl.pallas_call(
        functools.partial(place_kernel, n=n, chunks=chunks),
        out_shape=jax.ShapeDtypeStruct(shape, jnp.float32),
        grid_spec=pltpu.PrefetchScalarGridSpec(
            num_scalar_prefetch=1, grid=(),
            in_specs=[HBM] * (n + len(extra)),
            out_specs=HBM,
            scratch_shapes=[pltpu.VMEM((rows, cols), jnp.float32)] * n + [pltpu.SemaphoreType.DMA((n, chunks)), pltpu.SemaphoreType.DMA((chunks,))]),
        input_output_aliases={} if out is None else {1 + n: 0},
        compiler_params=pltpu.CompilerParams(vmem_limit_bytes=VMEM_LIMIT),
        cost_estimate=pl.CostEstimate(flops=rows * cols * 200, bytes_accessed=8 * rows * cols, transcendentals=0),
        name="place",
    )(at, *blocks, *extra)


def solution(mesh):
    n_dp = mesh.shape['dp']

    def hop(x, bit):
        return lax.ppermute(x, 'dp', [(i, i ^ bit) for i in range(n_dp)])

    def hop_tp(x):
        return lax.ppermute(x, 'tp', [(0, 1), (1, 0)])

    CORE, X, Y = 1, 2, 4

    def local_step(h_main, h_mtp, labels_main, labels_mtp, weight_main, weight_mtp, gain_final, gain_mtp, w_out):
        rows, d_model = h_main.shape[1:]
        shard_vocab = w_out.shape[1]
        q = rows // 4
        tp = lax.axis_index('tp')
        dp = lax.axis_index('dp')
        core = dp % 2
        chip = dp // 2
        vocab_start = tp * shard_vocab
        col_tile = jnp.minimum(chip * BLOCK_COLS, shard_vocab - BLOCK_COLS) // NARROW
        start = jnp.stack([vocab_start, col_tile]).astype(jnp.int32)
        gains = jnp.stack([gain_final, gain_mtp])

        labels = jnp.concatenate([labels_main, labels_mtp])
        weights = jnp.concatenate([weight_main, weight_mtp])
        small_all = lax.all_gather(jnp.stack([labels.astype(jnp.float32), weights]), 'dp')
        weight_sums = jnp.sum(small_all[:, 1], axis=(0, 2))
        loss_coefs = jnp.stack([1.0 / weight_sums[0], MTP_LAMBDA / weight_sums[1]])
        row_w_all = small_all[:, 1] * loss_coefs[None, :, None]
        labels_all = small_all[:, 0].astype(jnp.int32)
        row_w = (weights * loss_coefs[:, None]).reshape(2 * rows)
        labels = labels.reshape(2 * rows, 1)

        u_own, near, c0, c1a, c1b = run_norm(tp.reshape(1).astype(jnp.int32), h_main, h_mtp, gains, small_all)
        nx, ny = hop(near, X), hop(near, Y)
        c0x, c0y = hop(c0, X), hop(c0, Y)
        c1ax, c1ay = hop(c1a, X), hop(c1a, Y)
        c1bx, c1by = hop(c1b, X), hop(c1b, Y)
        nd = hop(ny, X)
        c0d = hop(c0x, Y)
        c1ad = hop(c1ay, X)
        c1bd = hop(c1bx, Y)
        zx, zy, zd = hop_tp(nx), hop_tp(ny), hop_tp(nd)
        pieces = {X: (nx, c0x, c1ax, c1bx, zx), Y: (ny, c0y, c1ay, c1by, zy), X | Y: (nd, c0d, c1ad, c1bd, zd)}

        z0, stats0 = run_logits(start, u_own, w_out, labels, u_own, 0, rows)
        z1, stats1 = run_logits(start, u_own, w_out, labels, stats0, 1, rows)
        stats = jnp.concatenate([stats0, stats1], axis=1).reshape(3, 2 * rows)
        other = hop_tp(stats)
        row_max = jnp.maximum(stats[0], other[0])
        row_sum = stats[1] * jnp.exp(stats[0] - row_max) + other[1] * jnp.exp(other[0] - row_max)
        log_norm = row_max + jnp.log(row_sum)
        loss_part = jnp.sum(row_w * (log_norm - (stats[2] + other[2])))
        norms = {d: hop(log_norm, d) for d in (X, Y, X | Y)}

        norm_col, w_col = log_norm.reshape(2 * rows, 1), row_w.reshape(2 * rows, 1)
        e_cls, u_cls = run_own_e(start, z0, z1, u_own, norm_col, w_col, labels)
        part0 = run_du(start, z0, w_out, norm_col, w_col, labels, stats1, 0, rows)
        other0 = hop_tp(part0)

        def order(v):
            v = v.reshape(2, rows)
            a, b = v[:, :q].reshape(2 * q), v[:, q:2 * q].reshape(2 * q)
            first, last = jnp.where(tp == 0, a, b), jnp.where(tp == 0, b, a)
            return jnp.concatenate([first, v[:, 2 * q:].reshape(2 * rows - 4 * q), last]).reshape(2 * rows, 1)

        dep = e_cls
        for slot, d in enumerate((X, Y, X | Y)):
            pick = lambda v: order(lax.dynamic_index_in_dim(v, dp ^ d, 0, keepdims=False))
            e_cls, u_cls = run_class_e(start, pieces[d], w_out, order(norms[d]), pick(row_w_all), pick(labels_all), e_cls, u_cls, slot + 1)

        blk = d_model // n_dp
        recv = []
        for d in (X | Y, X, Y, 0):
            where = jnp.stack([core, chip ^ (d // 2)]).astype(jnp.int32)
            keep, give = run_grad_w(where, u_cls, e_cls, dep)
            got = hop(give, CORE)
            if d == 0:
                recv.append((keep, got))
                break
            dep = keep + got
            recv.append((hop(dep, d),))
            if d == X:
                part1 = run_du(start, z1, w_out, norm_col, w_col, labels, keep, 1, rows)
                other1 = hop_tp(part1)
        gh0, gg0 = run_norm_back(h_main, part0, other0, gains[:1], keep)
        out, after = None, gg0
        for d, blocks in zip((0, X | Y, X, Y), (recv[3], recv[0], recv[1], recv[2])):
            src = chip ^ (d // 2)
            at = (jnp.minimum(src * BLOCK_COLS, shard_vocab - BLOCK_COLS) // NARROW).reshape(1).astype(jnp.int32)
            out = run_place(at, blocks, out, after, (blk, shard_vocab))
            if d == X:
                gh1, gg1 = run_norm_back(h_mtp, part1, other1, gains[1:], gg0)
                loss_total, grad_gain = lax.psum((loss_part, jnp.concatenate([gg0, gg1])), 'dp')
                after = grad_gain
        return loss_total, gh0, gh1, out, grad_gain[0], grad_gain[1]


    row_spec = P('dp', None)
    return jax.shard_map(local_step, mesh=mesh, in_specs=(P('dp', None, None), P('dp', None, None), row_spec, row_spec, row_spec, row_spec, P(None), P(None), P(None, 'tp')), out_specs=(P(), P('dp', None, None), P('dp', None, None), P('dp', 'tp'), P(None), P(None)), check_vma=False)
```

```python
import functools

import jax
import jax.numpy as jnp
from jax import lax
from jax.experimental import pallas as pl
from jax.experimental.pallas import tpu as pltpu
from jax.sharding import PartitionSpec as P


NORM_EPS = 1e-6
MTP_LAMBDA = 0.3
BLOCK_COLS = 4096
TILE = 2304
L_TILE = 768
NARROW = 256
VMEM_LIMIT = 60 * 1024 * 1024
CHAIN = ("60", "61", "20", "40", "21", "41", "00")
DU1_AFTER = "20"
NN = (((1,), (0,)), ((), ()))
NT = (((1,), (1,)), ((), ()))


def params(*semantics):
    return pltpu.CompilerParams(dimension_semantics=semantics, vmem_limit_bytes=VMEM_LIMIT)


HBM = pl.BlockSpec(memory_space=pl.ANY)


def norm_kernel(tp_ref, h0_ref, h1_ref, gain_ref, u_ref, near_ref, third_ref, *last_refs):
    head, b = pl.program_id(0), pl.program_id(1)

    def rows_of(h_ref):
        x = h_ref[0].astype(jnp.float32)
        return x * lax.rsqrt(jnp.mean(x * x, axis=-1, keepdims=True) + NORM_EPS)

    for i, h_ref in enumerate((h0_ref, h1_ref)):
        @pl.when(head == i)
        def _():
            u = rows_of(h_ref) * gain_ref[i:i + 1, :]
            u_ref[...] = u.astype(jnp.bfloat16)

            @pl.when(b == tp_ref[0])
            def _():
                near_ref[...] = u

            @pl.when(b == 2)
            def _():
                third_ref[...] = u

            @pl.when(b == 3)
            def _():
                last_refs[i][...] = u


def run_norm(tp, h0, h1, gains):
    _, rows, d = h0.shape
    q = rows // 4
    f32 = jnp.float32
    blk = lambda f: pl.BlockSpec((q, d), f)
    return pl.pallas_call(
        norm_kernel,
        out_shape=(jax.ShapeDtypeStruct((8 * rows, d), jnp.bfloat16), jax.ShapeDtypeStruct((2 * q, d), f32), jax.ShapeDtypeStruct((2 * q, d), f32), jax.ShapeDtypeStruct((q, d), f32), jax.ShapeDtypeStruct((q, d), f32)),
        grid_spec=pltpu.PrefetchScalarGridSpec(
            num_scalar_prefetch=1, grid=(2, 4),
            in_specs=[pl.BlockSpec((1, q, d), lambda h, b, s: (0, jnp.where(h == 0, b, 3), 0)), pl.BlockSpec((1, q, d), lambda h, b, s: (0, jnp.where(h == 0, 0, b), 0)), pl.BlockSpec((2, d), lambda h, b, s: (0, 0))],
            out_specs=(blk(lambda h, b, s: (4 * h + b, 0)), blk(lambda h, b, s: (h, 0)), blk(lambda h, b, s: (h, 0)), blk(lambda h, b, s: (0, 0)), blk(lambda h, b, s: (0, 0)))),
        compiler_params=params("arbitrary", "arbitrary"),
        cost_estimate=pl.CostEstimate(flops=8 * rows * d * 1000, bytes_accessed=14 * rows * d, transcendentals=rows),
        name="norm",
    )(tp, h0, h1, gains)


def norm_back_kernel(h_ref, a_ref, b_ref, gain_ref, _, out_ref, gg_ref):
    @pl.when(pl.program_id(0) == 0)
    def _():
        gg_ref[...] = jnp.zeros_like(gg_ref)

    x = h_ref[0].astype(jnp.float32)
    inv = lax.rsqrt(jnp.mean(x * x, axis=-1, keepdims=True) + NORM_EPS)
    normed = x * inv
    gu = a_ref[...] + b_ref[...]
    gn = gu * gain_ref[...]
    prod = gu * normed
    gg_ref[...] += jnp.sum(prod, axis=0, keepdims=True)
    gx = inv * (gn - normed * jnp.mean(gn * normed, axis=-1, keepdims=True))
    out_ref[0] = gx.astype(jnp.bfloat16)


def run_norm_back(h, a, b, gain, dep):
    _, rows, d = h.shape
    q = 128
    row = pl.BlockSpec((q, d), lambda i: (i, 0))
    row3 = pl.BlockSpec((1, q, d), lambda i: (0, i, 0))
    one = pl.BlockSpec((1, d), lambda i: (0, 0))
    return pl.pallas_call(
        norm_back_kernel,
        out_shape=(jax.ShapeDtypeStruct(h.shape, jnp.bfloat16), jax.ShapeDtypeStruct((1, d), jnp.float32)),
        grid=(rows // q,),
        in_specs=[row3, row, row, one, HBM],
        out_specs=(row3, one),
        compiler_params=params("arbitrary"),
        cost_estimate=pl.CostEstimate(flops=8 * rows * d * 1000, bytes_accessed=12 * rows * d, transcendentals=rows),
        name="norm_back",
    )(h, a, b, gain, dep)


def logits_kernel(start_ref, u_ref, w_ref, lab_ref, z_ref, stat_ref, m_ref, s_ref, t_ref, off_ref, *, sub):
    j = pl.program_id(0)
    rows, tile = z_ref.shape
    lanes = 128

    @pl.when(j == 0)
    def _():
        m_ref[...] = jnp.full_like(m_ref, -jnp.inf)
        s_ref[...] = jnp.zeros_like(s_ref)
        t_ref[...] = jnp.zeros_like(t_ref)
        off_ref[...] = label_offset(lab_ref[...], start_ref[0])

    base = j * tile
    z_ref[...] = lax.dot_general(u_ref[...], w_ref[...], NN, preferred_element_type=jnp.float32)
    for i in range(rows // sub):
        r = pl.ds(i * sub, sub)
        z = z_ref[r, :]
        parts = [z[:, k * lanes:(k + 1) * lanes] for k in range(tile // lanes)]
        m_old = m_ref[r, :]
        m_new = m_old
        for p in parts:
            m_new = jnp.maximum(m_new, p)
        off = off_ref[r, :] - base
        total = s_ref[r, :] * jnp.exp(m_old - m_new)
        target = t_ref[r, :]
        for k, p in enumerate(parts):
            total += jnp.exp(p - m_new)
            target = jnp.where(off == k * lanes, p, target)
        m_ref[r, :] = m_new
        s_ref[r, :] = total
        t_ref[r, :] = target

    @pl.when(j == pl.num_programs(0) - 1)
    def _():
        for i in range(0, rows, 128):
            r = pl.ds(i, 128)
            m = m_ref[r, :].T
            top = jnp.max(m, axis=0, keepdims=True)
            stat_ref[0:1, r] = top
            stat_ref[1:2, r] = jnp.sum(s_ref[r, :].T * jnp.exp(m - top), axis=0, keepdims=True)
            stat_ref[2:3, r] = jnp.sum(t_ref[r, :].T, axis=0, keepdims=True)


def run_logits(start, u, w, lab, rows):
    d, cols = w.shape
    full = lambda j, s: (0, 0)
    return pl.pallas_call(
        functools.partial(logits_kernel, sub=128),
        out_shape=(jax.ShapeDtypeStruct((rows, cols), jnp.float32), jax.ShapeDtypeStruct((3, rows), jnp.float32)),
        grid_spec=pltpu.PrefetchScalarGridSpec(
            num_scalar_prefetch=1, grid=(cols // L_TILE,),
            in_specs=[pl.BlockSpec((rows, d), full), pl.BlockSpec((d, L_TILE), lambda j, s: (0, j)), pl.BlockSpec((1, rows), full)],
            out_specs=(pl.BlockSpec((rows, L_TILE), lambda j, s: (0, j)), pl.BlockSpec((3, rows), full)),
            scratch_shapes=[pltpu.VMEM((rows, 128), jnp.float32)] * 3 + [pltpu.VMEM((rows, 128), jnp.int32)]),
        compiler_params=params("arbitrary"),
        cost_estimate=pl.CostEstimate(flops=2 * rows * d * cols, bytes_accessed=cols * (2 * d + 4 * rows), transcendentals=rows * cols),
        name="logits",
    )(start, u, w, lab)


def e_tile(z, shift, weight, off):
    parts = []
    for k in range(z.shape[1] // 128):
        p = jnp.exp(z[:, k * 128:(k + 1) * 128] - shift)
        parts.append(jnp.where(off == k * 128, p - weight, p))
    return jnp.concatenate(parts, axis=1).astype(jnp.bfloat16)


def spread(row):
    parts = [jnp.broadcast_to(row[:, i:i + 128], (128, 128)).T for i in range(0, row.shape[1], 128)]
    return jnp.concatenate(parts, axis=0)


def label_offset(row, vocab_start):
    lab = spread(row).astype(jnp.int32)
    return lab - vocab_start - lax.broadcasted_iota(jnp.int32, lab.shape, 1)


def fill_rows(start_ref, info_ref, shift_ref, weight_ref, off_ref):
    shift_ref[...] = spread(info_ref[0:1, :] - jnp.log(info_ref[1:2, :]))
    weight_ref[...] = spread(info_ref[1:2, :])
    off_ref[...] = label_offset(info_ref[2:3, :], start_ref[0])


def row_scratch(rows):
    return [pltpu.VMEM((rows, 128), jnp.float32), pltpu.VMEM((rows, 128), jnp.float32), pltpu.VMEM((rows, 128), jnp.int32)]


def du_kernel(start_ref, z_ref, w_ref, info_ref, _, out_ref, acc_ref, shift_ref, weight_ref, off_ref):
    j = pl.program_id(0)

    @pl.when(j == 0)
    def _():
        acc_ref[...] = jnp.zeros_like(acc_ref)
        fill_rows(start_ref, info_ref, shift_ref, weight_ref, off_ref)

    e = e_tile(z_ref[...], shift_ref[...], weight_ref[...], off_ref[...] - j * z_ref.shape[1])
    acc_ref[...] += lax.dot_general(e, w_ref[...], NT, preferred_element_type=jnp.float32)

    @pl.when(j == pl.num_programs(0) - 1)
    def _():
        out_ref[...] = acc_ref[...].astype(jnp.bfloat16).astype(jnp.float32)


def run_du(start, z, w, info, dep, head, rows):
    d, cols = w.shape
    steps = cols // TILE
    vec = pl.BlockSpec((info.shape[0], rows), lambda j, s: (0, head))
    return pl.pallas_call(
        du_kernel,
        out_shape=jax.ShapeDtypeStruct((rows, d), jnp.float32),
        grid_spec=pltpu.PrefetchScalarGridSpec(
            num_scalar_prefetch=1, grid=(steps,),
            in_specs=[pl.BlockSpec((rows, TILE), lambda j, s: (head, j)), pl.BlockSpec((d, TILE), lambda j, s: (0, j)), vec, HBM],
            out_specs=pl.BlockSpec((rows, d), lambda j, s: (0, 0)),
            scratch_shapes=[pltpu.VMEM((rows, d), jnp.float32)] + row_scratch(rows)),
        compiler_params=params("arbitrary"),
        cost_estimate=pl.CostEstimate(flops=2 * rows * d * cols, bytes_accessed=cols * (2 * d + 4 * rows), transcendentals=rows * cols),
        name="du",
    )(start, z, w, info, dep)


def own_e_kernel(start_ref, z0_ref, z1_ref, info_ref, _, e_ref, shift_ref, weight_ref, off_ref):
    j = pl.program_id(0)

    @pl.when(j == 0)
    def _():
        fill_rows(start_ref, info_ref, shift_ref, weight_ref, off_ref)

    for k, z_ref in enumerate((z0_ref, z1_ref)):
        at = (start_ref[1] + 2 * j + k) * NARROW
        e_ref[:, k * NARROW:(k + 1) * NARROW] = e_tile(z_ref[...], shift_ref[...], weight_ref[...], off_ref[...] - at)


def run_own_e(start, z, info, dep):
    rows = info.shape[1]
    vec = pl.BlockSpec(info.shape, lambda j, s: (0, 0))
    z_even = pl.BlockSpec((rows, NARROW), lambda j, s: (0, s[1] + 2 * j))
    z_odd = pl.BlockSpec((rows, NARROW), lambda j, s: (0, s[1] + 2 * j + 1))
    return pl.pallas_call(
        own_e_kernel,
        out_shape=jax.ShapeDtypeStruct((4 * rows, BLOCK_COLS), jnp.bfloat16),
        grid_spec=pltpu.PrefetchScalarGridSpec(
            num_scalar_prefetch=1, grid=(BLOCK_COLS // (2 * NARROW),),
            in_specs=[z_even, z_odd, vec, HBM],
            out_specs=pl.BlockSpec((rows, 2 * NARROW), lambda j, s: (0, j)),
            scratch_shapes=row_scratch(rows)),
        compiler_params=params("arbitrary"),
        cost_estimate=pl.CostEstimate(flops=rows * BLOCK_COLS * 2048, bytes_accessed=rows * 6 * BLOCK_COLS, transcendentals=rows * BLOCK_COLS),
        name="own_e",
    )(start, z, z, info, dep)


def class_e_kernel(start_ref, *refs, quarter, slot):
    n = len(refs) - 11
    pieces, (w_ref, info_ref, _, _, _, e_ref, u_ref, token_ref, shift_ref, weight_ref, off_ref) = refs[:n], refs[n:]
    j = pl.program_id(0)
    rows = e_ref.shape[0]

    @pl.when(j == 0)
    def _():
        at = 0
        for p in pieces:
            u_ref[at:at + p.shape[0], :] = p[...].astype(jnp.bfloat16)
            at += p.shape[0]
        fill_rows(start_ref, info_ref, shift_ref, weight_ref, off_ref)
        token_ref[...] = jnp.zeros_like(token_ref)

    used = start_ref[1 + slot]
    at = (start_ref[1] + 2 * j) * NARROW
    for count in (2, 3, 4):
        @pl.when(used == count)
        def _():
            r = slice(0, count * quarter)
            z = lax.dot_general(u_ref[r, :], w_ref[...], NN, preferred_element_type=jnp.float32)
            e_ref[r, :] = e_tile(z, shift_ref[r, :], weight_ref[r, :], off_ref[r, :] - at)
            if count < 4:
                e_ref[count * quarter:, :] = jnp.zeros((rows - count * quarter, e_ref.shape[1]), e_ref.dtype)


def run_class_e(start, pieces, w, info, e_all, u_all, dep, slot):
    d = w.shape[0]
    rows = sum(p.shape[0] for p in pieces)
    full = lambda j, s: (0, 0)
    once = pl.Buffered(1)
    n = len(pieces)
    return pl.pallas_call(
        functools.partial(class_e_kernel, quarter=rows // 4, slot=slot),
        out_shape=(jax.ShapeDtypeStruct(e_all.shape, e_all.dtype), jax.ShapeDtypeStruct(u_all.shape, u_all.dtype), jax.ShapeDtypeStruct((8, 128), jnp.float32)),
        grid_spec=pltpu.PrefetchScalarGridSpec(
            num_scalar_prefetch=1, grid=(BLOCK_COLS // (2 * NARROW),),
            in_specs=[pl.BlockSpec(p.shape, full, pipeline_mode=once) for p in pieces] + [pl.BlockSpec((pl.Element(d), pl.Element(2 * NARROW)), lambda j, s: (0, pl.multiple_of((s[1] + 2 * j) * NARROW, NARROW))), pl.BlockSpec(info.shape, full), HBM, HBM, HBM],
            out_specs=(pl.BlockSpec((rows, 2 * NARROW), lambda j, s: (slot, j)), pl.BlockSpec((rows, d), lambda j, s: (slot, 0)), pl.BlockSpec((8, 128), full)),
            scratch_shapes=row_scratch(rows)),
        input_output_aliases={1 + n + 2: 0, 1 + n + 3: 1},
        compiler_params=params("arbitrary"),
        cost_estimate=pl.CostEstimate(flops=2 * rows * d * BLOCK_COLS, bytes_accessed=BLOCK_COLS * 2 * (d + rows) + 6 * rows * d, transcendentals=rows * BLOCK_COLS),
        name="class_e",
    )(start, *pieces, w, info, e_all, u_all, dep)


def grad_w_kernel(start_ref, u_ref, e_ref, _, *refs):
    *before, ut_ref = refs
    if len(before) == 5:
        mine_ref, got_ref, keep_ref, give_ref, total_ref = before
        total_ref[...] = mine_ref[...] + got_ref[...]
    else:
        keep_ref, give_ref = before

    @pl.when(pl.program_id(0) == 0)
    def _():
        ut_ref[...] = u_ref[...].T

    g = lax.dot_general(ut_ref[...], e_ref[...], NN, preferred_element_type=jnp.float32)
    half = g.shape[0] // 2

    @pl.when(start_ref[0] == 0)
    def _():
        keep_ref[...] = g[:half]
        give_ref[...] = g[half:]

    @pl.when(start_ref[0] == 1)
    def _():
        keep_ref[...] = g[half:]
        give_ref[...] = g[:half]


def run_grad_w(where, u_all, e_all, dep, part, parts, previous=()):
    rows, cols = e_all.shape
    cols //= parts
    blk, tn = 512, 512
    first = part * (cols // tn)
    out = pl.BlockSpec((blk // 2, tn), lambda j, s: (0, j))
    n_out = 3 if previous else 2
    return pl.pallas_call(
        grad_w_kernel,
        out_shape=(jax.ShapeDtypeStruct((blk // 2, cols), jnp.float32),) * n_out,
        grid_spec=pltpu.PrefetchScalarGridSpec(
            num_scalar_prefetch=1, grid=(cols // tn,),
            in_specs=[pl.BlockSpec((rows, blk), lambda j, s: (0, s[1])), pl.BlockSpec((rows, tn), lambda j, s: (0, first + j)), HBM] + [out] * len(previous),
            out_specs=(out,) * n_out,
            scratch_shapes=[pltpu.VMEM((blk, rows), jnp.bfloat16)]),
        compiler_params=params("arbitrary"),
        cost_estimate=pl.CostEstimate(flops=2 * rows * blk * cols, bytes_accessed=2 * rows * (blk + cols) + 4 * blk * cols, transcendentals=0),
        name="grad_w",
    )(where, u_all, e_all, dep, *previous)


def place_kernel(at_ref, *refs, sizes, chunks):
    n = sum(sizes)
    blocks, (out_ref, *bufs, in_sem, out_sem) = refs[:n], refs[len(refs) - n - 3:]

    def load(i, k):
        width = blocks[i].shape[1] // chunks
        c = pl.ds(k * width, width)
        return pltpu.make_async_copy(blocks[i].at[:, c], bufs[i].at[:, c], in_sem.at[i, k])

    def store(g, i, k):
        width = blocks[i].shape[1] // chunks
        to = pl.ds(pl.multiple_of(at_ref[g] * NARROW + k * width, NARROW), width)
        return pltpu.make_async_copy(bufs[i].at[:, pl.ds(k * width, width)], out_ref.at[:, to], out_sem.at[i, k])

    for i in range(n):
        for k in range(chunks):
            load(i, k).start()
    i = 0
    for g, size in enumerate(sizes):
        for k in range(chunks):
            for m in range(size):
                load(i + m, k).wait()
            if size == 2:
                width = blocks[i].shape[1] // chunks
                c = slice(k * width, (k + 1) * width)
                bufs[i][:, c] += bufs[i + 1][:, c]
            store(g, i, k).start()
        i += size
    i = 0
    for g, size in enumerate(sizes):
        for k in range(chunks):
            store(g, i, k).wait()
        i += size


def run_place(at, groups, out, dep, shape):
    blocks = [b for g in groups for b in g]
    n, chunks = len(blocks), 2
    extra = [dep] if out is None else [out, dep]
    words = sum(b.size for b in blocks)
    return pl.pallas_call(
        functools.partial(place_kernel, sizes=tuple(len(g) for g in groups), chunks=chunks),
        out_shape=jax.ShapeDtypeStruct(shape, jnp.float32),
        grid_spec=pltpu.PrefetchScalarGridSpec(
            num_scalar_prefetch=1, grid=(),
            in_specs=[HBM] * (n + len(extra)),
            out_specs=HBM,
            scratch_shapes=[pltpu.VMEM(b.shape, jnp.float32) for b in blocks] + [pltpu.SemaphoreType.DMA((n, chunks)), pltpu.SemaphoreType.DMA((n, chunks))]),
        input_output_aliases={} if out is None else {1 + n: 0},
        compiler_params=pltpu.CompilerParams(vmem_limit_bytes=VMEM_LIMIT),
        cost_estimate=pl.CostEstimate(flops=words * 200, bytes_accessed=8 * words, transcendentals=0),
        name="place",
    )(at, *blocks, *extra)


def solution(mesh):
    n_dp = mesh.shape['dp']

    def hop(x, bit):
        return lax.ppermute(x, 'dp', [(i, i ^ bit) for i in range(n_dp)])

    def hop_tp(x):
        return lax.ppermute(x, 'tp', [(0, 1), (1, 0)])

    CORE, X, Y = 1, 2, 4

    def local_step(h_main, h_mtp, labels_main, labels_mtp, weight_main, weight_mtp, gain_final, gain_mtp, w_out):
        rows, d_model = h_main.shape[1:]
        shard_vocab = w_out.shape[1]
        q = rows // 4
        tp = lax.axis_index('tp')
        dp = lax.axis_index('dp')
        core = dp % 2
        chip = dp // 2
        vocab_start = tp * shard_vocab
        col_tile = jnp.minimum(chip * BLOCK_COLS, shard_vocab - BLOCK_COLS) // NARROW
        start = jnp.stack([vocab_start, col_tile]).astype(jnp.int32)
        gains = jnp.stack([gain_final, gain_mtp])

        labels = jnp.concatenate([labels_main, labels_mtp])
        weights = jnp.concatenate([weight_main, weight_mtp])
        weight_sums = jnp.sum(weights, axis=1)
        weight_sums = weight_sums + hop(weight_sums, CORE)
        weight_sums = weight_sums + hop(weight_sums, X) + hop(weight_sums, Y) + hop(weight_sums, X | Y)
        loss_coefs = jnp.stack([1.0 / weight_sums[0], MTP_LAMBDA / weight_sums[1]])
        row_w = (weights * loss_coefs[:, None]).reshape(2 * rows)
        labels = labels.reshape(2 * rows).astype(jnp.float32)

        u_cls, near, c0, c1a, c1b = run_norm(tp.reshape(1).astype(jnp.int32), h_main, h_mtp, gains)
        nx, ny = hop(near, X), hop(near, Y)
        c0x, c0y = hop(c0, X), hop(c0, Y)
        c1ax, c1ay = hop(c1a, X), hop(c1a, Y)
        c1bx, c1by = hop(c1b, X), hop(c1b, Y)
        nd = hop(ny, X)
        c0d = hop(c0x, Y)
        c1ad = hop(c1ay, X)
        c1bd = hop(c1bx, Y)
        zx, zy, zd = hop_tp(nx), hop_tp(ny), hop_tp(nd)
        pieces = {X: (nx, zx, c0x, c1ax, c1bx), Y: (ny, zy, c0y, c1ay, c1by), X | Y: (nd, zd, c0d, c1ad, c1bd)}

        z, stats = run_logits(start, u_cls, w_out, labels[None], 2 * rows)
        other = hop_tp(stats)
        row_max = jnp.maximum(stats[0], other[0])
        row_sum = stats[1] * jnp.exp(stats[0] - row_max) + other[1] * jnp.exp(other[0] - row_max)
        log_norm = row_max + jnp.log(row_sum)
        loss_part = jnp.sum(row_w * (log_norm - (stats[2] + other[2])))

        live = jnp.any(weights.reshape(2, 4, q) > 0, axis=(0, 2))
        used = jnp.where(live[3], 4.0, jnp.where(live[2], 3.0, 2.0))
        info = jnp.stack([log_norm, row_w, labels, jnp.broadcast_to(used, row_w.shape)])
        v = info.reshape(4, 2, 4, q)
        a, b = v[:, :, 0], v[:, :, 1]
        near_far = jnp.stack([jnp.where(tp == 0, a, b), jnp.where(tp == 0, b, a)], axis=1)
        info_sent = jnp.concatenate([near_far, jnp.swapaxes(v[:, :, 2:], 1, 2)], axis=1).reshape(4, 2 * rows)
        infos = {d: hop(info_sent, d) for d in (X, Y, X | Y)}
        start_all = jnp.concatenate([start, jnp.stack([infos[d][3, 0] for d in (X, Y, X | Y)]).astype(jnp.int32)])

        part0 = run_du(start, z, w_out, info, stats, 0, rows)
        other0 = hop_tp(part0)
        e_cls = run_own_e(start, z, info, part0)

        token = part0
        for slot, d in enumerate((X, Y, X | Y)):
            e_cls, u_cls, token = run_class_e(start_all, pieces[d], w_out, infos[d], e_cls, u_cls, token, slot + 1)

        blk = d_model // n_dp
        recv = {}
        dep, previous, send = token, (), None
        for tag in CHAIN:
            d, part = int(tag[0]), int(tag[1])
            where = jnp.stack([core, chip ^ (d // 2)]).astype(jnp.int32)
            last = d == 0
            keep, give, *total = run_grad_w(where, u_cls, e_cls, dep, part, 1 if last else 2, previous)
            if send:
                recv[send] = (hop(total[0], int(send[0])),)
            got = hop(give, CORE)
            previous, send, dep = (keep, got), tag, keep
            if last:
                recv[tag] = (keep, got)
            elif tag == CHAIN[-2]:
                dep = keep + got
                recv[tag] = (hop(dep, d),)
                previous, send = (), None
            elif tag == DU1_AFTER:
                part1 = run_du(start, z, w_out, info, keep, 1, rows)
                other1 = hop_tp(part1)
                dep = part1
        gh0, gg0 = run_norm_back(h_main, part0, other0, gains[:1], keep)
        gh1, gg1 = run_norm_back(h_mtp, part1, other1, gains[1:], gg0)
        sums = jnp.concatenate([gg0.reshape(-1), gg1.reshape(-1), jnp.broadcast_to(loss_part, (128,))])
        for bit in (CORE, X, Y):
            sums = sums + hop(sums, bit)
        loss_total, grad_gain = sums[2 * d_model], sums[:2 * d_model].reshape(2, d_model)

        def place(tags, out, after):
            at = []
            for tag in tags:
                src = chip ^ (int(tag[0]) // 2)
                at.append((jnp.minimum(src * BLOCK_COLS, shard_vocab - BLOCK_COLS) + int(tag[1]) * (BLOCK_COLS // 2)) // NARROW)
            return run_place(jnp.stack(at).astype(jnp.int32), [recv[t] for t in tags], out, after, (blk, shard_vocab))

        out = place(("00", "60", "61", "20", "40"), None, gg1)
        out = place(CHAIN[-3:-1], out, gg1)
        return loss_total, gh0, gh1, out, grad_gain[0], grad_gain[1]


    row_spec = P('dp', None)
    return jax.shard_map(local_step, mesh=mesh, in_specs=(P('dp', None, None), P('dp', None, None), row_spec, row_spec, row_spec, row_spec, P(None), P(None), P(None, 'tp')), out_specs=(P(), P('dp', None, None), P('dp', None, None), P('dp', 'tp'), P(None), P(None)), check_vma=False)
```

```python
import functools

import jax
import jax.numpy as jnp
from jax import lax
from jax.experimental import pallas as pl
from jax.experimental.pallas import tpu as pltpu
from jax.sharding import PartitionSpec as P


NORM_EPS = 1e-6
MTP_LAMBDA = 0.3
BLOCK_COLS = 4096
TILE = 1792
L_TILE = 768
NARROW = 256
VMEM_LIMIT = 60 * 1024 * 1024
CHAIN = ("60", "61", "20", "40", "21", "41", "00")
NN = (((1,), (0,)), ((), ()))
NT = (((1,), (1,)), ((), ()))


def params(*semantics):
    return pltpu.CompilerParams(dimension_semantics=semantics, vmem_limit_bytes=VMEM_LIMIT)


HBM = pl.BlockSpec(memory_space=pl.ANY)


def norm_kernel(tp_ref, h0_ref, h1_ref, gain_ref, u_ref, near_ref, third_ref, last_ref):
    head, b = pl.program_id(0), pl.program_id(1)

    def rows_of(h_ref):
        x = h_ref[0].astype(jnp.float32)
        return x * lax.rsqrt(jnp.mean(x * x, axis=-1, keepdims=True) + NORM_EPS)

    for i, h_ref in enumerate((h0_ref, h1_ref)):
        @pl.when(head == i)
        def _():
            u = rows_of(h_ref) * gain_ref[i:i + 1, :]
            u_ref[...] = u.astype(jnp.bfloat16)

            @pl.when(b == tp_ref[0])
            def _():
                near_ref[...] = u

            @pl.when(b == 2)
            def _():
                third_ref[...] = u

            @pl.when(b == 3)
            def _():
                last_ref[...] = u


def run_norm(tp, h0, h1, gains):
    _, rows, d = h0.shape
    q = rows // 4
    f32 = jnp.float32
    blk = lambda f: pl.BlockSpec((q, d), f)
    return pl.pallas_call(
        norm_kernel,
        out_shape=(jax.ShapeDtypeStruct((8 * rows, d), jnp.bfloat16), jax.ShapeDtypeStruct((2 * q, d), f32), jax.ShapeDtypeStruct((2 * q, d), f32), jax.ShapeDtypeStruct((2 * q, d), f32)),
        grid_spec=pltpu.PrefetchScalarGridSpec(
            num_scalar_prefetch=1, grid=(2, 4),
            in_specs=[pl.BlockSpec((1, q, d), lambda h, b, s: (0, jnp.where(h == 0, b, 3), 0)), pl.BlockSpec((1, q, d), lambda h, b, s: (0, jnp.where(h == 0, 0, b), 0)), pl.BlockSpec((2, d), lambda h, b, s: (0, 0))],
            out_specs=(blk(lambda h, b, s: (4 * h + b, 0)), blk(lambda h, b, s: (h, 0)), blk(lambda h, b, s: (h, 0)), blk(lambda h, b, s: (h, 0)))),
        compiler_params=params("arbitrary", "arbitrary"),
        cost_estimate=pl.CostEstimate(flops=8 * rows * d * 1000, bytes_accessed=14 * rows * d, transcendentals=rows),
        name="norm",
    )(tp, h0, h1, gains)


def norm_back_kernel(h_ref, a_ref, b_ref, gain_ref, _, out_ref, gg_ref):
    @pl.when(pl.program_id(0) == 0)
    def _():
        gg_ref[...] = jnp.zeros_like(gg_ref)

    x = h_ref[0].astype(jnp.float32)
    inv = lax.rsqrt(jnp.mean(x * x, axis=-1, keepdims=True) + NORM_EPS)
    normed = x * inv
    gu = a_ref[...] + b_ref[...]
    gn = gu * gain_ref[...]
    prod = gu * normed
    gg_ref[...] += jnp.sum(prod, axis=0, keepdims=True)
    gx = inv * (gn - normed * jnp.mean(gn * normed, axis=-1, keepdims=True))
    out_ref[0] = gx.astype(jnp.bfloat16)


def run_norm_back(h, a, b, gain, head, dep):
    _, rows, d = h.shape
    q = 128
    row = pl.BlockSpec((q, d), lambda i: (head * (rows // q) + i, 0))
    row3 = pl.BlockSpec((1, q, d), lambda i: (0, i, 0))
    one = pl.BlockSpec((1, d), lambda i: (0, 0))
    return pl.pallas_call(
        norm_back_kernel,
        out_shape=(jax.ShapeDtypeStruct(h.shape, jnp.bfloat16), jax.ShapeDtypeStruct((1, d), jnp.float32)),
        grid=(rows // q,),
        in_specs=[row3, row, row, one, HBM],
        out_specs=(row3, one),
        compiler_params=params("arbitrary"),
        cost_estimate=pl.CostEstimate(flops=8 * rows * d * 1000, bytes_accessed=12 * rows * d, transcendentals=rows),
        name="norm_back",
    )(h, a, b, gain, dep)


def logits_kernel(start_ref, u_ref, w_ref, lab_ref, z_ref, stat_ref, m_ref, s_ref, t_ref, off_ref, *, sub):
    j = pl.program_id(0)
    rows, tile = z_ref.shape
    lanes = 128

    @pl.when(j == 0)
    def _():
        m_ref[...] = jnp.full_like(m_ref, -jnp.inf)
        s_ref[...] = jnp.zeros_like(s_ref)
        t_ref[...] = jnp.zeros_like(t_ref)
        off_ref[...] = label_offset(lab_ref[...], start_ref[0])

    base = j * tile
    for i in range(rows // sub):
        r = pl.ds(i * sub, sub)
        z = lax.dot_general(u_ref[r, :], w_ref[...], NN, preferred_element_type=jnp.float32)
        z_ref[r, :] = z
        parts = [z[:, k * lanes:(k + 1) * lanes] for k in range(tile // lanes)]
        m_old = m_ref[r, :]
        m_new = m_old
        for p in parts:
            m_new = jnp.maximum(m_new, p)
        off = off_ref[r, :] - base
        total = s_ref[r, :] * jnp.exp(m_old - m_new)
        target = t_ref[r, :]
        for k, p in enumerate(parts):
            total += jnp.exp(p - m_new)
            target = jnp.where(off == k * lanes, p, target)
        m_ref[r, :] = m_new
        s_ref[r, :] = total
        t_ref[r, :] = target

    @pl.when(j == pl.num_programs(0) - 1)
    def _():
        for i in range(0, rows, 128):
            r = pl.ds(i, 128)
            m = m_ref[r, :].T
            top = jnp.max(m, axis=0, keepdims=True)
            stat_ref[0:1, r] = top
            stat_ref[1:2, r] = jnp.sum(s_ref[r, :].T * jnp.exp(m - top), axis=0, keepdims=True)
            stat_ref[2:3, r] = jnp.sum(t_ref[r, :].T, axis=0, keepdims=True)


def run_logits(start, u, w, lab, rows):
    d, cols = w.shape
    full = lambda j, s: (0, 0)
    return pl.pallas_call(
        functools.partial(logits_kernel, sub=256),
        out_shape=(jax.ShapeDtypeStruct((rows, cols), jnp.float32), jax.ShapeDtypeStruct((3, rows), jnp.float32)),
        grid_spec=pltpu.PrefetchScalarGridSpec(
            num_scalar_prefetch=1, grid=(cols // L_TILE,),
            in_specs=[pl.BlockSpec((rows, d), full), pl.BlockSpec((d, L_TILE), lambda j, s: (0, j)), pl.BlockSpec((1, rows), full)],
            out_specs=(pl.BlockSpec((rows, L_TILE), lambda j, s: (0, j)), pl.BlockSpec((3, rows), full)),
            scratch_shapes=[pltpu.VMEM((rows, 128), jnp.float32)] * 3 + [pltpu.VMEM((rows, 128), jnp.int32)]),
        compiler_params=params("arbitrary"),
        cost_estimate=pl.CostEstimate(flops=2 * rows * d * cols, bytes_accessed=cols * (2 * d + 4 * rows), transcendentals=rows * cols),
        name="logits",
    )(start, u, w, lab)


def e_tile(z, shift, weight, off):
    parts = []
    for k in range(z.shape[1] // 128):
        p = jnp.exp(z[:, k * 128:(k + 1) * 128] - shift)
        parts.append(jnp.where(off == k * 128, p - weight, p))
    return jnp.concatenate(parts, axis=1).astype(jnp.bfloat16)


def spread(row):
    parts = [jnp.broadcast_to(row[:, i:i + 128], (128, 128)).T for i in range(0, row.shape[1], 128)]
    return jnp.concatenate(parts, axis=0)


def label_offset(row, vocab_start):
    lab = spread(row).astype(jnp.int32)
    return lab - vocab_start - lax.broadcasted_iota(jnp.int32, lab.shape, 1)


def fill_rows(start_ref, info_ref, shift_ref, weight_ref, off_ref):
    shift_ref[...] = spread(info_ref[0:1, :] - jnp.log(info_ref[1:2, :]))
    weight_ref[...] = spread(info_ref[1:2, :])
    off_ref[...] = label_offset(info_ref[2:3, :], start_ref[0])


def row_scratch(rows):
    return [pltpu.VMEM((rows, 128), jnp.float32), pltpu.VMEM((rows, 128), jnp.float32), pltpu.VMEM((rows, 128), jnp.int32)]


def du_kernel(start_ref, z_ref, w_ref, info_ref, out_ref, e_ref, shift_ref, weight_ref, off_ref):
    j = pl.program_id(0)
    tile = z_ref.shape[1]

    @pl.when(j == 0)
    def _():
        out_ref[...] = jnp.zeros_like(out_ref)
        fill_rows(start_ref, info_ref, shift_ref, weight_ref, off_ref)

    e = e_tile(z_ref[...], shift_ref[...], weight_ref[...], off_ref[...] - j * tile)
    out_ref[...] += lax.dot_general(e, w_ref[...], NT, preferred_element_type=jnp.float32)

    for k in range(tile // NARROW):
        at = j * (tile // NARROW) + k - start_ref[1]

        @pl.when((at >= 0) & (at < BLOCK_COLS // NARROW))
        def _():
            e_ref[:, pl.ds(pl.multiple_of(at * NARROW, NARROW), NARROW)] = e[:, k * NARROW:(k + 1) * NARROW]

    @pl.when(j == pl.num_programs(0) - 1)
    def _():
        out_ref[...] = out_ref[...].astype(jnp.bfloat16).astype(jnp.float32)


def run_du(start, z, w, info):
    d, cols = w.shape
    rows = info.shape[1]
    full = lambda j, s: (0, 0)
    once = pl.Buffered(1)
    return pl.pallas_call(
        du_kernel,
        out_shape=(jax.ShapeDtypeStruct((rows, d), jnp.float32), jax.ShapeDtypeStruct((4 * rows, BLOCK_COLS), jnp.bfloat16)),
        grid_spec=pltpu.PrefetchScalarGridSpec(
            num_scalar_prefetch=1, grid=(cols // TILE,),
            in_specs=[pl.BlockSpec((rows, TILE), lambda j, s: (0, j)), pl.BlockSpec((d, TILE), lambda j, s: (0, j)), pl.BlockSpec(info.shape, full)],
            out_specs=(pl.BlockSpec((rows, d), full, pipeline_mode=once), pl.BlockSpec((rows, BLOCK_COLS), full, pipeline_mode=once)),
            scratch_shapes=row_scratch(rows)),
        compiler_params=params("arbitrary"),
        cost_estimate=pl.CostEstimate(flops=2 * rows * d * cols, bytes_accessed=cols * (2 * d + 4 * rows), transcendentals=rows * cols),
        name="du",
    )(start, z, w, info)


def class_e_kernel(start_ref, *refs, quarter):
    n = len(refs) - 12
    pieces, (w_ref, info_ref, _, _, _, e_ref, u_ref, token_ref, shift_ref, weight_ref, off_ref, used_ref) = refs[:n], refs[n:]
    j = pl.program_id(0)
    rows = e_ref.shape[0]

    @pl.when(j == 0)
    def _():
        at = 0
        for p in pieces:
            u_ref[at:at + p.shape[0], :] = p[...].astype(jnp.bfloat16)
            at += p.shape[0]
        fill_rows(start_ref, info_ref, shift_ref, weight_ref, off_ref)
        token_ref[...] = jnp.zeros_like(token_ref)
        used_ref[0] = jnp.max(info_ref[3:4, :]).astype(jnp.int32)

    used = used_ref[0]
    at = (start_ref[1] + 2 * j) * NARROW
    for count in (2, 3, 4):
        @pl.when(used == count)
        def _():
            r = slice(0, count * quarter)

            def columns(c, at):
                z = lax.dot_general(u_ref[r, :], w_ref[:, c], NN, preferred_element_type=jnp.float32)
                e_ref[r, c] = e_tile(z, shift_ref[r, :], weight_ref[r, :], off_ref[r, :] - at)

            if count == 4:
                columns(slice(0, 2 * NARROW), at)
            else:
                @pl.loop(0, 2)
                def _(i):
                    columns(pl.ds(pl.multiple_of(i * NARROW, NARROW), NARROW), at + i * NARROW)

            if count < 4:
                e_ref[count * quarter:, :] = jnp.zeros((rows - count * quarter, e_ref.shape[1]), e_ref.dtype)


def run_class_e(start, pieces, w, info, e_all, u_all, dep, slot):
    d = w.shape[0]
    rows = sum(p.shape[0] for p in pieces)
    full = lambda j, s: (0, 0)
    once = pl.Buffered(1)
    n = len(pieces)
    return pl.pallas_call(
        functools.partial(class_e_kernel, quarter=rows // 4),
        out_shape=(jax.ShapeDtypeStruct(e_all.shape, e_all.dtype), jax.ShapeDtypeStruct(u_all.shape, u_all.dtype), jax.ShapeDtypeStruct((8, 128), jnp.float32)),
        grid_spec=pltpu.PrefetchScalarGridSpec(
            num_scalar_prefetch=1, grid=(BLOCK_COLS // (2 * NARROW),),
            in_specs=[pl.BlockSpec(p.shape, full, pipeline_mode=once) for p in pieces] + [pl.BlockSpec((pl.Element(d), pl.Element(2 * NARROW)), lambda j, s: (0, pl.multiple_of((s[1] + 2 * j) * NARROW, NARROW))), pl.BlockSpec(info.shape, full), HBM, HBM, HBM],
            out_specs=(pl.BlockSpec((rows, 2 * NARROW), lambda j, s: (slot, j)), pl.BlockSpec((rows, d), lambda j, s: (slot, 0)), pl.BlockSpec((8, 128), full)),
            scratch_shapes=row_scratch(rows) + [pltpu.SMEM((1,), jnp.int32)]),
        input_output_aliases={1 + n + 2: 0, 1 + n + 3: 1},
        compiler_params=params("arbitrary"),
        cost_estimate=pl.CostEstimate(flops=2 * rows * d * BLOCK_COLS, bytes_accessed=BLOCK_COLS * 2 * (d + rows) + 6 * rows * d, transcendentals=rows * BLOCK_COLS),
        name="class_e",
    )(start, *pieces, w, info, e_all, u_all, dep)


def grad_w_kernel(start_ref, u_ref, e_ref, _, *refs):
    *before, ut_ref = refs
    if len(before) == 5:
        mine_ref, got_ref, keep_ref, give_ref, total_ref = before
        total_ref[...] = mine_ref[...] + got_ref[...]
    else:
        keep_ref, give_ref = before

    @pl.when(pl.program_id(0) == 0)
    def _():
        @pl.loop(0, u_ref.shape[0] // 512)
        def _(i):
            r = pl.ds(pl.multiple_of(i * 512, 512), 512)
            ut_ref[:, r] = u_ref[r, :].T

    half = ut_ref.shape[0] // 2

    @pl.loop(0, e_ref.shape[1] // NARROW)
    def _(i):
        c = pl.ds(pl.multiple_of(i * NARROW, NARROW), NARROW)
        g = lax.dot_general(ut_ref[...], e_ref[:, c], NN, preferred_element_type=jnp.float32)

        @pl.when(start_ref[0] == 0)
        def _():
            keep_ref[:, c] = g[:half]
            give_ref[:, c] = g[half:]

        @pl.when(start_ref[0] == 1)
        def _():
            keep_ref[:, c] = g[half:]
            give_ref[:, c] = g[:half]


def run_grad_w(where, u_all, e_all, dep, part, parts, previous=()):
    rows, cols = e_all.shape
    cols //= parts
    blk, tn = 512, 512
    first = part * (cols // tn)
    out = pl.BlockSpec((blk // 2, tn), lambda j, s: (0, j))
    n_out = 3 if previous else 2
    return pl.pallas_call(
        grad_w_kernel,
        out_shape=(jax.ShapeDtypeStruct((blk // 2, cols), jnp.float32),) * n_out,
        grid_spec=pltpu.PrefetchScalarGridSpec(
            num_scalar_prefetch=1, grid=(cols // tn,),
            in_specs=[pl.BlockSpec((rows, blk), lambda j, s: (0, s[1])), pl.BlockSpec((rows, tn), lambda j, s: (0, first + j)), HBM] + [out] * len(previous),
            out_specs=(out,) * n_out,
            scratch_shapes=[pltpu.VMEM((blk, rows), jnp.bfloat16)]),
        compiler_params=params("arbitrary"),
        cost_estimate=pl.CostEstimate(flops=2 * rows * blk * cols, bytes_accessed=2 * rows * (blk + cols) + 4 * blk * cols, transcendentals=0),
        name="grad_w",
    )(where, u_all, e_all, dep, *previous)


def place_kernel(at_ref, *refs, sizes, chunks):
    n = sum(sizes)
    blocks, (out_ref, *bufs, in_sem, out_sem) = refs[:n], refs[len(refs) - n - 3:]

    def load(i, k):
        width = blocks[i].shape[1] // chunks
        c = pl.ds(k * width, width)
        return pltpu.make_async_copy(blocks[i].at[:, c], bufs[i].at[:, c], in_sem.at[i, k])

    def store(g, i, k):
        width = blocks[i].shape[1] // chunks
        to = pl.ds(pl.multiple_of(at_ref[g] * NARROW + k * width, NARROW), width)
        return pltpu.make_async_copy(bufs[i].at[:, pl.ds(k * width, width)], out_ref.at[:, to], out_sem.at[i, k])

    for i in range(n):
        for k in range(chunks):
            load(i, k).start()
    i = 0
    for g, size in enumerate(sizes):
        for k in range(chunks):
            for m in range(size):
                load(i + m, k).wait()
            if size == 2:
                width = blocks[i].shape[1] // chunks
                c = slice(k * width, (k + 1) * width)
                bufs[i][:, c] += bufs[i + 1][:, c]
            store(g, i, k).start()
        i += size
    i = 0
    for g, size in enumerate(sizes):
        for k in range(chunks):
            store(g, i, k).wait()
        i += size


def run_place(at, groups, out, dep, shape):
    blocks = [b for g in groups for b in g]
    n, chunks = len(blocks), 2
    extra = [dep] if out is None else [out, dep]
    words = sum(b.size for b in blocks)
    return pl.pallas_call(
        functools.partial(place_kernel, sizes=tuple(len(g) for g in groups), chunks=chunks),
        out_shape=jax.ShapeDtypeStruct(shape, jnp.float32),
        grid_spec=pltpu.PrefetchScalarGridSpec(
            num_scalar_prefetch=1, grid=(),
            in_specs=[HBM] * (n + len(extra)),
            out_specs=HBM,
            scratch_shapes=[pltpu.VMEM(b.shape, jnp.float32) for b in blocks] + [pltpu.SemaphoreType.DMA((n, chunks)), pltpu.SemaphoreType.DMA((n, chunks))]),
        input_output_aliases={} if out is None else {1 + n: 0},
        compiler_params=pltpu.CompilerParams(vmem_limit_bytes=VMEM_LIMIT),
        cost_estimate=pl.CostEstimate(flops=words * 200, bytes_accessed=8 * words, transcendentals=0),
        name="place",
    )(at, *blocks, *extra)


def solution(mesh):
    n_dp = mesh.shape['dp']

    def hop(x, bit):
        return lax.ppermute(x, 'dp', [(i, i ^ bit) for i in range(n_dp)])

    def hop_tp(x):
        return lax.ppermute(x, 'tp', [(0, 1), (1, 0)])

    CORE, X, Y = 1, 2, 4

    def local_step(h_main, h_mtp, labels_main, labels_mtp, weight_main, weight_mtp, gain_final, gain_mtp, w_out):
        rows, d_model = h_main.shape[1:]
        shard_vocab = w_out.shape[1]
        q = rows // 4
        tp = lax.axis_index('tp')
        dp = lax.axis_index('dp')
        core = dp % 2
        chip = dp // 2
        vocab_start = tp * shard_vocab
        col_tile = jnp.minimum(chip * BLOCK_COLS, shard_vocab - BLOCK_COLS) // NARROW
        start = jnp.stack([vocab_start, col_tile]).astype(jnp.int32)
        gains = jnp.stack([gain_final, gain_mtp])

        labels = jnp.concatenate([labels_main, labels_mtp])
        weights = jnp.concatenate([weight_main, weight_mtp])
        weight_sums = jnp.sum(weights, axis=1)
        weight_sums = weight_sums + hop(weight_sums, CORE)
        weight_sums = weight_sums + hop(weight_sums, X) + hop(weight_sums, Y) + hop(weight_sums, X | Y)
        loss_coefs = jnp.stack([1.0 / weight_sums[0], MTP_LAMBDA / weight_sums[1]])
        row_w = (weights * loss_coefs[:, None]).reshape(2 * rows)
        labels = labels.reshape(2 * rows).astype(jnp.float32)

        u_cls, near, c0, c1 = run_norm(tp.reshape(1).astype(jnp.int32), h_main, h_mtp, gains)
        nx, ny = hop(near, X), hop(near, Y)
        c0x, c0y = hop(c0, X), hop(c0, Y)
        c1x, c1y = hop(c1, X), hop(c1, Y)
        nd = hop(ny, X)
        c0d = hop(c0x, Y)
        c1d = hop(c1, X | Y)
        zx, zy, zd = hop_tp(nx), hop_tp(ny), hop_tp(nd)
        pieces = {X: (nx, zx, c0x, c1x), Y: (ny, zy, c0y, c1y), X | Y: (nd, zd, c0d, c1d)}

        z, stats = run_logits(start, u_cls, w_out, labels[None], 2 * rows)
        other = hop_tp(stats)
        row_max = jnp.maximum(stats[0], other[0])
        row_sum = stats[1] * jnp.exp(stats[0] - row_max) + other[1] * jnp.exp(other[0] - row_max)
        log_norm = row_max + jnp.log(row_sum)
        loss_part = jnp.sum(row_w * (log_norm - (stats[2] + other[2])))

        live = jnp.any(weights.reshape(2, 4, q) > 0, axis=(0, 2))
        used = jnp.where(live[3], 4.0, jnp.where(live[2], 3.0, 2.0))
        info = jnp.stack([log_norm, row_w, labels, jnp.broadcast_to(used, row_w.shape)])
        v = info.reshape(4, 2, 4, q)
        a, b = v[:, :, 0], v[:, :, 1]
        near_far = jnp.stack([jnp.where(tp == 0, a, b), jnp.where(tp == 0, b, a)], axis=1)
        info_sent = jnp.concatenate([near_far, jnp.swapaxes(v[:, :, 2:], 1, 2)], axis=1).reshape(4, 2 * rows)
        infos = {d: hop(info_sent, d) for d in (X, Y, X | Y)}

        part, e_cls = run_du(start, z, w_out, info)
        other = hop_tp(part)
        token = stats
        for slot, d in enumerate((X, Y, X | Y)):
            e_cls, u_cls, token = run_class_e(start, pieces[d], w_out, infos[d], e_cls, u_cls, token, slot + 1)

        blk = d_model // n_dp
        recv = {}
        dep, previous, send = token, (), None
        for tag in CHAIN:
            d, half = int(tag[0]), int(tag[1])
            where = jnp.stack([core, chip ^ (d // 2)]).astype(jnp.int32)
            last = d == 0
            keep, give, *total = run_grad_w(where, u_cls, e_cls, dep, half, 1 if last else 2, previous)
            if send:
                recv[send] = (hop(total[0], int(send[0])),)
            got = hop(give, CORE)
            previous, send, dep = (keep, got), tag, keep
            if last:
                recv[tag] = (keep, got)
            elif tag in (CHAIN[0], CHAIN[-2]):
                dep = keep + got
                recv[tag] = (hop(dep, d),)
                previous, send = (), None
        gh0, gg0 = run_norm_back(h_main, part, other, gains[:1], 0, keep)
        gh1, gg1 = run_norm_back(h_mtp, part, other, gains[1:], 1, gg0)
        sums = jnp.concatenate([gg0.reshape(-1), gg1.reshape(-1), jnp.broadcast_to(loss_part, (128,))])
        for bit in (CORE, X, Y):
            sums = sums + hop(sums, bit)
        loss_total, grad_gain = sums[2 * d_model], sums[:2 * d_model].reshape(2, d_model)

        def place(tags, out, after):
            at = []
            for tag in tags:
                src = chip ^ (int(tag[0]) // 2)
                at.append((jnp.minimum(src * BLOCK_COLS, shard_vocab - BLOCK_COLS) + int(tag[1]) * (BLOCK_COLS // 2)) // NARROW)
            return run_place(jnp.stack(at).astype(jnp.int32), [recv[t] for t in tags], out, after, (blk, shard_vocab))

        out = place(("00", "60", "61", "20", "40"), None, gg1)
        out = place(CHAIN[-3:-1], out, gg1)
        return loss_total, gh0, gh1, out, grad_gain[0], grad_gain[1]


    row_spec = P('dp', None)
    return jax.shard_map(local_step, mesh=mesh, in_specs=(P('dp', None, None), P('dp', None, None), row_spec, row_spec, row_spec, row_spec, P(None), P(None), P(None, 'tp')), out_specs=(P(), P('dp', None, None), P('dp', None, None), P('dp', 'tp'), P(None), P(None)), check_vma=False)
```

```python
import functools

import jax
import jax.numpy as jnp
from jax import lax
from jax.experimental import pallas as pl
from jax.experimental.pallas import tpu as pltpu
from jax.sharding import PartitionSpec as P


NORM_EPS = 1e-6
MTP_LAMBDA = 0.3
BLOCK_COLS = 4096
TILE = 1792
L_TILE = 768
NARROW = 256
VMEM_LIMIT = 60 * 1024 * 1024
CHAIN = ("60", "61", "20", "40", "21", "41", "00")
NN = (((1,), (0,)), ((), ()))
NT = (((1,), (1,)), ((), ()))


def params(*semantics):
    return pltpu.CompilerParams(dimension_semantics=semantics, vmem_limit_bytes=VMEM_LIMIT)


HBM = pl.BlockSpec(memory_space=pl.ANY)


def norm_kernel(tp_ref, h0_ref, h1_ref, gain_ref, u_ref, near_ref, third_ref, last_ref):
    head, b = pl.program_id(0), pl.program_id(1)

    def rows_of(h_ref):
        x = h_ref[0].astype(jnp.float32)
        return x * lax.rsqrt(jnp.mean(x * x, axis=-1, keepdims=True) + NORM_EPS)

    for i, h_ref in enumerate((h0_ref, h1_ref)):
        @pl.when(head == i)
        def _():
            u = rows_of(h_ref) * gain_ref[i:i + 1, :]
            u_ref[...] = u.astype(jnp.bfloat16)

            @pl.when(b == tp_ref[0])
            def _():
                near_ref[...] = u

            @pl.when(b == 2)
            def _():
                third_ref[...] = u

            @pl.when(b == 3)
            def _():
                last_ref[...] = u


def run_norm(tp, h0, h1, gains):
    _, rows, d = h0.shape
    q = rows // 4
    f32 = jnp.float32
    blk = lambda f: pl.BlockSpec((q, d), f)
    return pl.pallas_call(
        norm_kernel,
        out_shape=(jax.ShapeDtypeStruct((8 * rows, d), jnp.bfloat16), jax.ShapeDtypeStruct((2 * q, d), f32), jax.ShapeDtypeStruct((2 * q, d), f32), jax.ShapeDtypeStruct((2 * q, d), f32)),
        grid_spec=pltpu.PrefetchScalarGridSpec(
            num_scalar_prefetch=1, grid=(2, 4),
            in_specs=[pl.BlockSpec((1, q, d), lambda h, b, s: (0, jnp.where(h == 0, b, 3), 0)), pl.BlockSpec((1, q, d), lambda h, b, s: (0, jnp.where(h == 0, 0, b), 0)), pl.BlockSpec((2, d), lambda h, b, s: (0, 0))],
            out_specs=(blk(lambda h, b, s: (4 * h + b, 0)), blk(lambda h, b, s: (h, 0)), blk(lambda h, b, s: (h, 0)), blk(lambda h, b, s: (h, 0)))),
        compiler_params=params("arbitrary", "arbitrary"),
        cost_estimate=pl.CostEstimate(flops=8 * rows * d * 1000, bytes_accessed=14 * rows * d, transcendentals=rows),
        name="norm",
    )(tp, h0, h1, gains)


def norm_back_kernel(h_ref, a_ref, b_ref, gain_ref, _, out_ref, gg_ref):
    @pl.when(pl.program_id(0) == 0)
    def _():
        gg_ref[...] = jnp.zeros_like(gg_ref)

    x = h_ref[0].astype(jnp.float32)
    inv = lax.rsqrt(jnp.mean(x * x, axis=-1, keepdims=True) + NORM_EPS)
    normed = x * inv
    gu = a_ref[...] + b_ref[...]
    gn = gu * gain_ref[...]
    prod = gu * normed
    gg_ref[...] += jnp.sum(prod, axis=0, keepdims=True)
    gx = inv * (gn - normed * jnp.mean(gn * normed, axis=-1, keepdims=True))
    out_ref[0] = gx.astype(jnp.bfloat16)


def run_norm_back(h, a, b, gain, head, dep):
    _, rows, d = h.shape
    q = 128
    row = pl.BlockSpec((q, d), lambda i: (head * (rows // q) + i, 0))
    row3 = pl.BlockSpec((1, q, d), lambda i: (0, i, 0))
    one = pl.BlockSpec((1, d), lambda i: (0, 0))
    return pl.pallas_call(
        norm_back_kernel,
        out_shape=(jax.ShapeDtypeStruct(h.shape, jnp.bfloat16), jax.ShapeDtypeStruct((1, d), jnp.float32)),
        grid=(rows // q,),
        in_specs=[row3, row, row, one, HBM],
        out_specs=(row3, one),
        compiler_params=params("arbitrary"),
        cost_estimate=pl.CostEstimate(flops=8 * rows * d * 1000, bytes_accessed=12 * rows * d, transcendentals=rows),
        name="norm_back",
    )(h, a, b, gain, dep)


def logits_kernel(start_ref, u_ref, w_ref, lab_ref, z_ref, stat_ref, m_ref, s_ref, t_ref, off_ref, *, sub):
    j = pl.program_id(0)
    rows, tile = z_ref.shape
    lanes = 128

    @pl.when(j == 0)
    def _():
        m_ref[...] = jnp.full_like(m_ref, -jnp.inf)
        s_ref[...] = jnp.zeros_like(s_ref)
        t_ref[...] = jnp.zeros_like(t_ref)
        off_ref[...] = label_offset(lab_ref[...], start_ref[0])

    base = j * tile
    for i in range(rows // sub):
        r = pl.ds(i * sub, sub)
        z = lax.dot_general(u_ref[r, :], w_ref[...], NN, preferred_element_type=jnp.float32)
        z_ref[r, :] = z
        parts = [z[:, k * lanes:(k + 1) * lanes] for k in range(tile // lanes)]
        m_old = m_ref[r, :]
        m_new = m_old
        for p in parts:
            m_new = jnp.maximum(m_new, p)
        off = off_ref[r, :] - base
        total = s_ref[r, :] * jnp.exp(m_old - m_new)
        target = t_ref[r, :]
        for k, p in enumerate(parts):
            total += jnp.exp(p - m_new)
            target = jnp.where(off == k * lanes, p, target)
        m_ref[r, :] = m_new
        s_ref[r, :] = total
        t_ref[r, :] = target

    @pl.when(j == pl.num_programs(0) - 1)
    def _():
        for i in range(0, rows, 128):
            r = pl.ds(i, 128)
            m = m_ref[r, :].T
            top = jnp.max(m, axis=0, keepdims=True)
            stat_ref[0:1, r] = top
            stat_ref[1:2, r] = jnp.sum(s_ref[r, :].T * jnp.exp(m - top), axis=0, keepdims=True)
            stat_ref[2:3, r] = jnp.sum(t_ref[r, :].T, axis=0, keepdims=True)


def run_logits(start, u, w, lab, rows):
    d, cols = w.shape
    full = lambda j, s: (0, 0)
    return pl.pallas_call(
        functools.partial(logits_kernel, sub=256),
        out_shape=(jax.ShapeDtypeStruct((rows, cols), jnp.float32), jax.ShapeDtypeStruct((3, rows), jnp.float32)),
        grid_spec=pltpu.PrefetchScalarGridSpec(
            num_scalar_prefetch=1, grid=(cols // L_TILE,),
            in_specs=[pl.BlockSpec((rows, d), full), pl.BlockSpec((d, L_TILE), lambda j, s: (0, j)), pl.BlockSpec((1, rows), full)],
            out_specs=(pl.BlockSpec((rows, L_TILE), lambda j, s: (0, j)), pl.BlockSpec((3, rows), full)),
            scratch_shapes=[pltpu.VMEM((rows, 128), jnp.float32)] * 3 + [pltpu.VMEM((rows, 128), jnp.int32)]),
        compiler_params=params("arbitrary"),
        cost_estimate=pl.CostEstimate(flops=2 * rows * d * cols, bytes_accessed=cols * (2 * d + 4 * rows), transcendentals=rows * cols),
        name="logits",
    )(start, u, w, lab)


def e_tile(z, shift, weight, off):
    parts = []
    for k in range(z.shape[1] // 128):
        p = jnp.exp(z[:, k * 128:(k + 1) * 128] - shift)
        parts.append(jnp.where(off == k * 128, p - weight, p))
    return jnp.concatenate(parts, axis=1).astype(jnp.bfloat16)


def spread(row):
    parts = [jnp.broadcast_to(row[:, i:i + 128], (128, 128)).T for i in range(0, row.shape[1], 128)]
    return jnp.concatenate(parts, axis=0)


def label_offset(row, vocab_start):
    lab = spread(row).astype(jnp.int32)
    return lab - vocab_start - lax.broadcasted_iota(jnp.int32, lab.shape, 1)


def fill_rows(start_ref, info_ref, shift_ref, weight_ref, off_ref):
    shift_ref[...] = spread(info_ref[0:1, :] - jnp.log(info_ref[1:2, :]))
    weight_ref[...] = spread(info_ref[1:2, :])
    off_ref[...] = label_offset(info_ref[2:3, :], start_ref[0])


def row_scratch(rows):
    return [pltpu.VMEM((rows, 128), jnp.float32), pltpu.VMEM((rows, 128), jnp.float32), pltpu.VMEM((rows, 128), jnp.int32)]


def du_kernel(start_ref, z_ref, w_ref, info_ref, out_ref, e_ref, shift_ref, weight_ref, off_ref):
    j = pl.program_id(0)
    tile = z_ref.shape[1]

    @pl.when(j == 0)
    def _():
        out_ref[...] = jnp.zeros_like(out_ref)
        fill_rows(start_ref, info_ref, shift_ref, weight_ref, off_ref)

    e = e_tile(z_ref[...], shift_ref[...], weight_ref[...], off_ref[...] - j * tile)
    out_ref[...] += lax.dot_general(e, w_ref[...], NT, preferred_element_type=jnp.float32)

    for k in range(tile // NARROW):
        at = j * (tile // NARROW) + k - start_ref[1]

        @pl.when((at >= 0) & (at < BLOCK_COLS // NARROW))
        def _():
            e_ref[:, pl.ds(pl.multiple_of(at * NARROW, NARROW), NARROW)] = e[:, k * NARROW:(k + 1) * NARROW]

    @pl.when(j == pl.num_programs(0) - 1)
    def _():
        out_ref[...] = out_ref[...].astype(jnp.bfloat16).astype(jnp.float32)


def run_du(start, z, w, info):
    d, cols = w.shape
    rows = info.shape[1]
    full = lambda j, s: (0, 0)
    once = pl.Buffered(1)
    return pl.pallas_call(
        du_kernel,
        out_shape=(jax.ShapeDtypeStruct((rows, d), jnp.float32), jax.ShapeDtypeStruct((4 * rows, BLOCK_COLS), jnp.bfloat16)),
        grid_spec=pltpu.PrefetchScalarGridSpec(
            num_scalar_prefetch=1, grid=(cols // TILE,),
            in_specs=[pl.BlockSpec((rows, TILE), lambda j, s: (0, j)), pl.BlockSpec((d, TILE), lambda j, s: (0, j)), pl.BlockSpec(info.shape, full)],
            out_specs=(pl.BlockSpec((rows, d), full, pipeline_mode=once), pl.BlockSpec((rows, BLOCK_COLS), full, pipeline_mode=once)),
            scratch_shapes=row_scratch(rows)),
        compiler_params=params("arbitrary"),
        cost_estimate=pl.CostEstimate(flops=2 * rows * d * cols, bytes_accessed=cols * (2 * d + 4 * rows), transcendentals=rows * cols),
        name="du",
    )(start, z, w, info)


def class_e_kernel(start_ref, *refs, quarter):
    n = len(refs) - 12
    pieces, (w_ref, info_ref, _, _, _, e_ref, u_ref, token_ref, shift_ref, weight_ref, off_ref, used_ref) = refs[:n], refs[n:]
    j = pl.program_id(0)
    rows = e_ref.shape[0]

    @pl.when(j == 0)
    def _():
        at = 0
        for p in pieces:
            u_ref[at:at + p.shape[0], :] = p[...].astype(jnp.bfloat16)
            at += p.shape[0]
        fill_rows(start_ref, info_ref, shift_ref, weight_ref, off_ref)
        token_ref[...] = jnp.zeros_like(token_ref)
        used_ref[0] = jnp.max(info_ref[3:4, :]).astype(jnp.int32)

    used = used_ref[0]
    at = (start_ref[1] + 2 * j) * NARROW
    for count in (2, 3, 4):
        @pl.when(used == count)
        def _():
            r = slice(0, count * quarter)

            def columns(c, at):
                z = lax.dot_general(u_ref[r, :], w_ref[:, c], NN, preferred_element_type=jnp.float32)
                e_ref[r, c] = e_tile(z, shift_ref[r, :], weight_ref[r, :], off_ref[r, :] - at)

            if count == 4:
                columns(slice(0, 2 * NARROW), at)
            else:
                @pl.loop(0, 2)
                def _(i):
                    columns(pl.ds(pl.multiple_of(i * NARROW, NARROW), NARROW), at + i * NARROW)

            if count < 4:
                e_ref[count * quarter:, :] = jnp.zeros((rows - count * quarter, e_ref.shape[1]), e_ref.dtype)


def run_class_e(start, pieces, w, info, e_all, u_all, dep, slot):
    d = w.shape[0]
    rows = sum(p.shape[0] for p in pieces)
    full = lambda j, s: (0, 0)
    once = pl.Buffered(1)
    n = len(pieces)
    return pl.pallas_call(
        functools.partial(class_e_kernel, quarter=rows // 4),
        out_shape=(jax.ShapeDtypeStruct(e_all.shape, e_all.dtype), jax.ShapeDtypeStruct(u_all.shape, u_all.dtype), jax.ShapeDtypeStruct((8, 128), jnp.float32)),
        grid_spec=pltpu.PrefetchScalarGridSpec(
            num_scalar_prefetch=1, grid=(BLOCK_COLS // (2 * NARROW),),
            in_specs=[pl.BlockSpec(p.shape, full, pipeline_mode=once) for p in pieces] + [pl.BlockSpec((pl.Element(d), pl.Element(2 * NARROW)), lambda j, s: (0, pl.multiple_of((s[1] + 2 * j) * NARROW, NARROW))), pl.BlockSpec(info.shape, full), HBM, HBM, HBM],
            out_specs=(pl.BlockSpec((rows, 2 * NARROW), lambda j, s: (slot, j)), pl.BlockSpec((rows, d), lambda j, s: (slot, 0)), pl.BlockSpec((8, 128), full)),
            scratch_shapes=row_scratch(rows) + [pltpu.SMEM((1,), jnp.int32)]),
        input_output_aliases={1 + n + 2: 0, 1 + n + 3: 1},
        compiler_params=params("arbitrary"),
        cost_estimate=pl.CostEstimate(flops=2 * rows * d * BLOCK_COLS, bytes_accessed=BLOCK_COLS * 2 * (d + rows) + 6 * rows * d, transcendentals=rows * BLOCK_COLS),
        name="class_e",
    )(start, *pieces, w, info, e_all, u_all, dep)


def grad_w_kernel(start_ref, u_ref, e_ref, _, *refs):
    *before, ut_ref = refs
    if len(before) == 5:
        mine_ref, got_ref, keep_ref, give_ref, total_ref = before
        total_ref[...] = mine_ref[...] + got_ref[...]
    else:
        keep_ref, give_ref = before

    @pl.when(pl.program_id(0) == 0)
    def _():
        @pl.loop(0, u_ref.shape[0] // 512)
        def _(i):
            r = pl.ds(pl.multiple_of(i * 512, 512), 512)
            ut_ref[:, r] = u_ref[r, :].T

    half = ut_ref.shape[0] // 2

    @pl.loop(0, e_ref.shape[1] // NARROW)
    def _(i):
        c = pl.ds(pl.multiple_of(i * NARROW, NARROW), NARROW)
        g = lax.dot_general(ut_ref[...], e_ref[:, c], NN, preferred_element_type=jnp.float32)

        @pl.when(start_ref[0] == 0)
        def _():
            keep_ref[:, c] = g[:half]
            give_ref[:, c] = g[half:]

        @pl.when(start_ref[0] == 1)
        def _():
            keep_ref[:, c] = g[half:]
            give_ref[:, c] = g[:half]


def run_grad_w(where, u_all, e_all, dep, part, parts, previous=()):
    rows, cols = e_all.shape
    cols //= parts
    blk, tn = 512, 512
    first = part * (cols // tn)
    out = pl.BlockSpec((blk // 2, tn), lambda j, s: (0, j))
    n_out = 3 if previous else 2
    return pl.pallas_call(
        grad_w_kernel,
        out_shape=(jax.ShapeDtypeStruct((blk // 2, cols), jnp.float32),) * n_out,
        grid_spec=pltpu.PrefetchScalarGridSpec(
            num_scalar_prefetch=1, grid=(cols // tn,),
            in_specs=[pl.BlockSpec((rows, blk), lambda j, s: (0, s[1])), pl.BlockSpec((rows, tn), lambda j, s: (0, first + j)), HBM] + [out] * len(previous),
            out_specs=(out,) * n_out,
            scratch_shapes=[pltpu.VMEM((blk, rows), jnp.bfloat16)]),
        compiler_params=params("arbitrary"),
        cost_estimate=pl.CostEstimate(flops=2 * rows * blk * cols, bytes_accessed=2 * rows * (blk + cols) + 4 * blk * cols, transcendentals=0),
        name="grad_w",
    )(where, u_all, e_all, dep, *previous)


def place_kernel(at_ref, *refs, sizes, chunks):
    n = sum(sizes)
    blocks, (out_ref, *bufs, in_sem, out_sem) = refs[:n], refs[len(refs) - n - 3:]

    def load(i, k):
        width = blocks[i].shape[1] // chunks
        c = pl.ds(k * width, width)
        return pltpu.make_async_copy(blocks[i].at[:, c], bufs[i].at[:, c], in_sem.at[i, k])

    def store(g, i, k):
        width = blocks[i].shape[1] // chunks
        to = pl.ds(pl.multiple_of(at_ref[g] * NARROW + k * width, NARROW), width)
        return pltpu.make_async_copy(bufs[i].at[:, pl.ds(k * width, width)], out_ref.at[:, to], out_sem.at[i, k])

    for i in range(n):
        for k in range(chunks):
            load(i, k).start()
    i = 0
    for g, size in enumerate(sizes):
        for k in range(chunks):
            for m in range(size):
                load(i + m, k).wait()
            if size == 2:
                width = blocks[i].shape[1] // chunks
                c = slice(k * width, (k + 1) * width)
                bufs[i][:, c] += bufs[i + 1][:, c]
            store(g, i, k).start()
        i += size
    i = 0
    for g, size in enumerate(sizes):
        for k in range(chunks):
            store(g, i, k).wait()
        i += size


def run_place(at, groups, out, dep, shape):
    blocks = [b for g in groups for b in g]
    n, chunks = len(blocks), 2
    extra = [dep] if out is None else [out, dep]
    words = sum(b.size for b in blocks)
    return pl.pallas_call(
        functools.partial(place_kernel, sizes=tuple(len(g) for g in groups), chunks=chunks),
        out_shape=jax.ShapeDtypeStruct(shape, jnp.float32),
        grid_spec=pltpu.PrefetchScalarGridSpec(
            num_scalar_prefetch=1, grid=(),
            in_specs=[HBM] * (n + len(extra)),
            out_specs=HBM,
            scratch_shapes=[pltpu.VMEM(b.shape, jnp.float32) for b in blocks] + [pltpu.SemaphoreType.DMA((n, chunks)), pltpu.SemaphoreType.DMA((n, chunks))]),
        input_output_aliases={} if out is None else {1 + n: 0},
        compiler_params=pltpu.CompilerParams(vmem_limit_bytes=VMEM_LIMIT),
        cost_estimate=pl.CostEstimate(flops=words * 200, bytes_accessed=8 * words, transcendentals=0),
        name="place",
    )(at, *blocks, *extra)


def solution(mesh):
    n_dp = mesh.shape['dp']

    def hop(x, bit):
        return lax.ppermute(x, 'dp', [(i, i ^ bit) for i in range(n_dp)])

    def hop_tp(x):
        return lax.ppermute(x, 'tp', [(0, 1), (1, 0)])

    CORE, X, Y = 1, 2, 4

    def local_step(h_main, h_mtp, labels_main, labels_mtp, weight_main, weight_mtp, gain_final, gain_mtp, w_out):
        rows, d_model = h_main.shape[1:]
        shard_vocab = w_out.shape[1]
        q = rows // 4
        tp = lax.axis_index('tp')
        dp = lax.axis_index('dp')
        core = dp % 2
        chip = dp // 2
        vocab_start = tp * shard_vocab
        col_tile = jnp.minimum(chip * BLOCK_COLS, shard_vocab - BLOCK_COLS) // NARROW
        start = jnp.stack([vocab_start, col_tile]).astype(jnp.int32)
        gains = jnp.stack([gain_final, gain_mtp])

        labels = jnp.concatenate([labels_main, labels_mtp])
        weights = jnp.concatenate([weight_main, weight_mtp])
        weight_sums = jnp.sum(weights, axis=1)
        weight_sums = weight_sums + hop(weight_sums, CORE)
        weight_sums = weight_sums + hop(weight_sums, X) + hop(weight_sums, Y) + hop(weight_sums, X | Y)
        loss_coefs = jnp.stack([1.0 / weight_sums[0], MTP_LAMBDA / weight_sums[1]])
        row_w = (weights * loss_coefs[:, None]).reshape(2 * rows)
        labels = labels.reshape(2 * rows).astype(jnp.float32)

        u_cls, near, c0, c1 = run_norm(tp.reshape(1).astype(jnp.int32), h_main, h_mtp, gains)
        nx, ny = hop(near, X), hop(near, Y)
        c0x, c0y = hop(c0, X), hop(c0, Y)
        c1x, c1y = hop(c1, X), hop(c1, Y)
        nd = hop(ny, X)
        c0d = hop(c0x, Y)
        c1d = hop(c1, X | Y)
        zx, zy, zd = hop_tp(nx), hop_tp(ny), hop_tp(nd)
        pieces = {X: (nx, zx, c0x, c1x), Y: (ny, zy, c0y, c1y), X | Y: (nd, zd, c0d, c1d)}

        z, stats = run_logits(start, u_cls, w_out, labels[None], 2 * rows)
        other = hop_tp(stats)
        row_max = jnp.maximum(stats[0], other[0])
        row_sum = stats[1] * jnp.exp(stats[0] - row_max) + other[1] * jnp.exp(other[0] - row_max)
        log_norm = row_max + jnp.log(row_sum)
        loss_part = jnp.sum(row_w * (log_norm - (stats[2] + other[2])))

        live = jnp.any(weights.reshape(2, 4, q) > 0, axis=(0, 2))
        used = jnp.where(live[3], 4.0, jnp.where(live[2], 3.0, 2.0))
        info = jnp.stack([log_norm, row_w, labels, jnp.broadcast_to(used, row_w.shape)])
        v = info.reshape(4, 2, 4, q)
        a, b = v[:, :, 0], v[:, :, 1]
        near_far = jnp.stack([jnp.where(tp == 0, a, b), jnp.where(tp == 0, b, a)], axis=1)
        info_sent = jnp.concatenate([near_far, jnp.swapaxes(v[:, :, 2:], 1, 2)], axis=1).reshape(4, 2 * rows)
        infos = {d: hop(info_sent, d) for d in (X, Y, X | Y)}

        part, e_cls = run_du(start, z, w_out, info)
        other = hop_tp(part)
        token = stats
        for slot, d in enumerate((X, Y, X | Y)):
            e_cls, u_cls, token = run_class_e(start, pieces[d], w_out, infos[d], e_cls, u_cls, token, slot + 1)

        blk = d_model // n_dp
        recv = {}
        dep, previous, send = token, (), None
        for tag in CHAIN:
            d, half = int(tag[0]), int(tag[1])
            where = jnp.stack([core, chip ^ (d // 2)]).astype(jnp.int32)
            last = d == 0
            keep, give, *total = run_grad_w(where, u_cls, e_cls, dep, half, 1 if last else 2, previous)
            if send:
                recv[send] = (hop(total[0], int(send[0])),)
            got = hop(give, CORE)
            previous, send, dep = (keep, got), tag, keep
            if last:
                recv[tag] = (keep, got)
            elif tag in (CHAIN[0], CHAIN[-2]):
                dep = keep + got
                recv[tag] = (hop(dep, d),)
                previous, send = (), None
                if tag == CHAIN[-2]:
                    gh0, gg0 = run_norm_back(h_main, part, other, gains[:1], 0, dep)
                    gh1, gg1 = run_norm_back(h_mtp, part, other, gains[1:], 1, gg0)
                    dep = gg1
        sums = jnp.concatenate([gg0.reshape(-1), gg1.reshape(-1), jnp.broadcast_to(loss_part, (128,))])
        for bit in (CORE, X, Y):
            sums = sums + hop(sums, bit)
        loss_total, grad_gain = sums[2 * d_model], sums[:2 * d_model].reshape(2, d_model)

        def place(tags, out, after):
            at = []
            for tag in tags:
                src = chip ^ (int(tag[0]) // 2)
                at.append((jnp.minimum(src * BLOCK_COLS, shard_vocab - BLOCK_COLS) + int(tag[1]) * (BLOCK_COLS // 2)) // NARROW)
            return run_place(jnp.stack(at).astype(jnp.int32), [recv[t] for t in tags], out, after, (blk, shard_vocab))

        out = place(("00", "60", "61", "20", "40"), None, keep)
        out = place(CHAIN[-3:-1], out, keep)
        return loss_total, gh0, gh1, out, grad_gain[0], grad_gain[1]


    row_spec = P('dp', None)
    return jax.shard_map(local_step, mesh=mesh, in_specs=(P('dp', None, None), P('dp', None, None), row_spec, row_spec, row_spec, row_spec, P(None), P(None), P(None, 'tp')), out_specs=(P(), P('dp', None, None), P('dp', None, None), P('dp', 'tp'), P(None), P(None)), check_vma=False)
```
